512 devices in a mesh: cols: 64 (over z, x, y_hi), rows: 8 (over y_lo, core).
Axes of the slice: x: 4, y: 8 (y_hi: 2, y_lo: 4; y = y_hi * 4 + y_lo), z: 8, core: 2. Of those that a mesh axis runs over, the one named last changes fastest.
Arguments:
- vectors: float32 [8192, 16384], P('rows', 'cols'), may hold values from -6 to 6
- reflectors: float32 [15, 1024, 512], P(None, None, 'cols'), may hold values from -40 to 40, as said below
- factors: float32 [15, 512, 512], P(None, None, 'cols'), may hold values from -1 to 1
Outputs:
- result: float32 [8192, 16384], P('rows', 'cols')
The draws below stay inside these ranges and needn't reach their ends.
Inputs may be any that keep to these rules, and one draw needn't show every extreme that they name: `reflectors`: column j of each block is zero outside its rows j to j + 511, and its entry in row j is 1.
All inputs are finite; a program needn't handle non-finite values.
Results may differ from the reference program's by a relative error of at most 0.00028.
Values sent between devices are 32-bit elements; how exact they have to be, the bound alone decides.
A program may use at most 64 MiB of HBM per device.

```python
import jax
import jax.numpy as jnp
from jax import lax

B = 512
BLOCKS = 15
NR = 8192
NC = 16384


def basis_draw(key):
    inner = jax.random.fold_in(key, 11)
    values = jax.random.normal(inner, (BLOCKS, 2 * B, B), jnp.float32)
    row_ids = lax.broadcasted_iota(jnp.int32, (2 * B, B), 0)
    col_ids = lax.broadcasted_iota(jnp.int32, (2 * B, B), 1)
    inside = (row_ids >= col_ids) & (row_ids < col_ids + B)
    leading = row_ids == col_ids
    banded = jnp.where(inside[None], values, jnp.float32(0.0))
    return jnp.where(leading[None], jnp.float32(1.0), banded)


def factor_from(basis_cols):
    gram = jnp.dot(basis_cols.T, basis_cols, precision=lax.Precision.HIGHEST, preferred_element_type=jnp.float32)
    upper = jnp.triu(gram, 1) + jnp.diag(jnp.diag(gram) * 0.5)
    return jnp.triu(jnp.linalg.inv(upper))


def draw_reflectors(key, part):
    return basis_draw(key)


def draw_factors(key, part):
    return jax.vmap(factor_from)(basis_draw(key))


def block_scale(own_key, dims, shards, least, high):
    factor_of, own = 1.0, jax.random.fold_in(own_key, 6)
    for dim, parts in shards:
        draws = jnp.exp(jax.random.uniform(jax.random.fold_in(own, dim), (parts,), jnp.float32, least / len(shards), high / len(shards)))
        factor_of = factor_of * jnp.repeat(draws, dims[dim] // parts).reshape([-1 if axis == dim else 1 for axis in range(len(dims))])
    return factor_of


def bell_draw(key, shape, scale, reach, pieces=(), dtype=jnp.bfloat16):
    drawn = jax.random.normal(key, shape, jnp.float32) * scale
    if len(pieces) > 0:
        drawn = block_scale(key, shape, pieces, -0.22, 0.18) * drawn
    return jnp.clip(drawn, min=-reach, max=reach).astype(dtype)


def setup_inputs(seed: int = 0) -> dict:
    key_list = jax.random.split(jax.random.key(seed), 4)
    return {
        "vectors": bell_draw(key_list[0], (NR, NC), 1.0, 6.0, ((0, 8), (1, 64)), jnp.float32),
        "reflectors": draw_reflectors(jax.random.fold_in(key_list[3], 71), 0),
        "factors": draw_factors(jax.random.fold_in(key_list[3], 71), 0),
    }


def reflect(window, basis_cols, factor):
    highest = lax.Precision.HIGHEST
    weights = jnp.dot(basis_cols.T.astype(jnp.float32), window.astype(jnp.float32), precision=highest, preferred_element_type=jnp.float32)
    coeffs = jnp.dot(factor.astype(jnp.float32), weights.astype(jnp.float32), precision=highest, preferred_element_type=jnp.float32)
    return window - jnp.dot(basis_cols.astype(jnp.float32), coeffs.astype(jnp.float32), precision=highest, preferred_element_type=jnp.float32)

def reference(vectors, reflectors, factors):

    def advance(index, matrix):
        start = (index * B).astype(jnp.int32)
        window = lax.dynamic_slice_in_dim(matrix, start, 2 * B, 0)
        basis_cols = lax.dynamic_index_in_dim(reflectors, index, 0, keepdims=False)
        factor = lax.dynamic_index_in_dim(factors, index, 0, keepdims=False)
        updated = reflect(window, basis_cols, factor)
        return lax.dynamic_update_slice_in_dim(matrix, updated, start, 0)
    return lax.fori_loop(0, BLOCKS, advance, vectors)
```

```python
import jax
import jax.numpy as jnp
from jax import lax
from jax.experimental import pallas as pl
from jax.experimental.pallas import tpu as pltpu
from jax.sharding import PartitionSpec as P

MESH = pl.DeviceIdType.MESH
F32, BF16 = jnp.float32, jnp.bfloat16
NZ, NX, NH = 8, 4, 2
B, HALF, N = 512, 256, 256
BAND = 640
LC = 128
STRIPES = B // LC
NN = (((1,), (0,)), ((), ()))
NT = (((1,), (1,)), ((), ()))
TN = (((0,), (0,)), ((), ()))


def split(v):
    hi = v.astype(BF16)
    return hi, (v - hi.astype(F32)).astype(BF16)


def dot3(a, b, dims=NN):
    def one(u, v):
        return lax.dot_general(u, v, dims, preferred_element_type=F32)

    return one(a[0], b[0]) + one(a[0], b[1]) + one(a[1], b[0])


def put(ref, at, v):
    hi, lo = split(v)
    ref[(0, *at)] = hi
    ref[(1, *at)] = lo


def get(ref, rows, cols):
    return ref[0, rows, cols], ref[1, rows, cols]


ALL, T0, T1 = slice(0, 512), slice(0, 256), slice(256, 512)


def times_lower(a, m, off=0):
    lo, hi = slice(off, off + 256), slice(off + 256, off + 512)
    left = dot3(get(a, slice(None), ALL), get(m, ALL, lo))
    right = dot3(get(a, slice(None), T1), get(m, T1, hi))
    return left, right


def times_upper(a, m):
    left = dot3(get(a, slice(None), T0), get(m, T0, T0))
    right = dot3(get(a, slice(None), ALL), get(m, ALL, T1))
    return left, right


def lower_lower(out, a, m, off=0):
    lo, hi = slice(off, off + 256), slice(off + 256, off + 512)
    put(out, (T0, T0), dot3(get(a, T0, T0), get(m, T0, lo)))
    put(out, (T1, T0), dot3(get(a, T1, ALL), get(m, ALL, lo)))
    put(out, (T1, T1), dot3(get(a, T1, T1), get(m, T1, hi)))


def kernel(
    vec, rft, fat, out,
    vt_buf, ft_buf, x_buf, xp_buf, d_buf, do_buf, ret_buf, ro_buf,
    xs, vs1, vs2, fs1, fs2, h1, h2, g, m, at, ds, ws, zs1, zs2,
    c1, c2, e, xt,
    lsem, p_s, p_r, vz_s, vz_r, vx_s, vx_r, fx_s, fx_r, fz_s, fz_r,
    xc_s, xc_r, d_s, d_r, ret_s, ret_r,
):
    c = lax.axis_index("cols")
    r = lax.axis_index("rows")
    z, x, h = c // (NX * NH), (c // NH) % NX, c % NH
    q = z // 2
    last = lax.axis_size("rows") - 1

    def at_c(zz, xx, hh):
        return (zz * NX + xx) * NH + hh

    zp, zm = at_c((z + 1) % NZ, x, h), at_c((z + NZ - 1) % NZ, x, h)
    xp, xm = at_c(z, (x + 1) % NX, h), at_c(z, (x + NX - 1) % NX, h)
    twin = at_c(z, x, 1 - h)
    b_first, b_own = jnp.maximum(2 * r - 1, 0), 2 * r
    zdir, xdir = (zp, zm), (xp, xm)

    own8 = pl.ds(pl.multiple_of(16 * x + 8 * h, 8), 8)
    lanes = pl.ds(pl.multiple_of(128 * q, 128), BAND)
    local = []
    for i, b in enumerate((b_first, b_own)):
        local.append(pltpu.make_async_copy(rft.at[b, :, lanes], vt_buf.at[i, z, own8, :], lsem.at[2 * i]))
        local.append(pltpu.make_async_copy(fat.at[b], ft_buf.at[i, z, own8, :], lsem.at[2 * i + 1]))
    xload = pltpu.make_async_copy(vec, x_buf, lsem.at[4])
    for cp in local:
        cp.start()
    xload.start()

    barrier = pltpu.get_barrier_semaphore()
    for cc in (zp, zm, xp, xm, twin):
        pl.semaphore_signal(barrier, inc=1, device_id=(cc, r), device_id_type=MESH)

    @pl.when(r > 0)
    def _():
        pl.semaphore_signal(barrier, inc=1, device_id=(c, r - 1), device_id_type=MESH)

    @pl.when(r < last)
    def _():
        pl.semaphore_signal(barrier, inc=1, device_id=(c, r + 1), device_id_type=MESH)

    pl.semaphore_wait(barrier, 5 + jnp.minimum(r, 1) + jnp.minimum(last - r, 1))

    sent = []

    def send(src, ssem, rsem, cc, rr=None, dst=None):
        cp = pltpu.make_async_remote_copy(
            src_ref=src, dst_ref=src if dst is None else dst, send_sem=ssem, recv_sem=rsem,
            device_id=(cc, r if rr is None else rr), device_id_type=MESH,
        )
        cp.start()
        sent.append(cp)

    def arrived(ref, ssem, rsem, cc):
        pltpu.make_async_remote_copy(
            src_ref=ref, dst_ref=ref, send_sem=ssem, recv_sem=rsem,
            device_id=(cc, r), device_id_type=MESH,
        ).wait_recv()

    for cp in local:
        cp.wait()
    send(vt_buf.at[:, z, own8, :], p_s.at[0], p_r.at[0], twin)
    send(ft_buf.at[:, z, own8, :], p_s.at[1], p_r.at[1], twin)
    xload.wait()

    @pl.when(r < last)
    def _():
        pltpu.make_async_remote_copy(
            src_ref=x_buf.at[pl.ds(B, B), :], dst_ref=xp_buf, send_sem=xc_s.at[0], recv_sem=xc_r.at[0],
            device_id=(c, r + 1), device_id_type=MESH,
        ).start()

    @pl.when(r == 0)
    def _():
        xp_buf[...] = jnp.zeros_like(xp_buf)
        d_buf[...] = jnp.zeros_like(d_buf)

    @pl.when(r == last)
    def _():
        ret_buf[...] = jnp.zeros_like(ret_buf)

    def rows16(xx):
        return pl.ds(pl.multiple_of(16 * xx, 16), 16)

    def vpiece(dz, xx, blk=slice(None)):
        return vt_buf.at[blk, (z + dz + NZ) % NZ, rows16(xx), :]

    def fslab(dz, blk):
        return ft_buf.at[blk, (z + dz + NZ) % NZ]

    def part(d):
        return pl.ds(d, 1)

    xnear = ((x + NX - 1) % NX, (x + 1) % NX)
    xfar = (x + 2) % NX
    other8 = pl.ds(pl.multiple_of(16 * x + 8 * (1 - h), 8), 8)

    def vz_send(s):
        for d in range(2):
            dz = -(s - 1) if d == 0 else s - 1
            ref = vpiece(dz, x) if s < 4 else vpiece(dz, x, part(d))
            send(ref, vz_s.at[d, s - 1], vz_r.at[d, s - 1], zdir[d])

    def vz_wait(s):
        for d in range(2):
            dz = -s if d == 0 else s
            ref = vpiece(dz, x) if s < 4 else vpiece(dz, x, part(d))
            arrived(ref, vz_s.at[d, s - 1], vz_r.at[d, s - 1], zdir[d])

    def vx_send1(dz):
        k = dz % NZ
        for d in range(2):
            send(vpiece(dz, x), vx_s.at[d, 0, k], vx_r.at[d, 0, k], xdir[d])

    def vx_send2(dz):
        k = dz % NZ
        for d in range(2):
            arrived(vpiece(dz, xnear[d]), vx_s.at[d, 0, k], vx_r.at[d, 0, k], xdir[d])
            send(vpiece(dz, xnear[d], part(d)), vx_s.at[d, 1, k], vx_r.at[d, 1, k], xdir[d])

    def vx_last(dz):
        k = dz % NZ
        for d in range(2):
            arrived(vpiece(dz, xfar, part(d)), vx_s.at[d, 1, k], vx_r.at[d, 1, k], xdir[d])

    def fz_send(s):
        for d in range(2):
            dz = -(s - 1) if d == 0 else s - 1
            for b in range(2) if s < 4 else (d,):
                send(fslab(dz, b), fz_s.at[d, b, s - 1], fz_r.at[d, b, s - 1], zdir[d])

    def fz_step(s):
        for b in range(2):
            for d in range(2):
                if s == 4 and b != d:
                    continue
                arrived(
                    fslab(-s if d == 0 else s, b), fz_s.at[d, b, s - 1], fz_r.at[d, b, s - 1], zdir[d]
                )
                if s < 3 or (s == 3 and b == d):
                    send(
                        fslab(-s if d == 0 else s, b), fz_s.at[d, b, s], fz_r.at[d, b, s], zdir[d]
                    )

    def fpiece(xx, blk=slice(None)):
        return ft_buf.at[blk, z, rows16(xx), :]

    arrived(vt_buf.at[:, z, other8, :], p_s.at[0], p_r.at[0], twin)
    vz_send(1)
    arrived(ft_buf.at[:, z, other8, :], p_s.at[1], p_r.at[1], twin)
    for d in range(2):
        send(fpiece(x), fx_s.at[d, 0], fx_r.at[d, 0], xdir[d])
    vx_send1(0)
    for d in range(2):
        arrived(fpiece(xnear[d]), fx_s.at[d, 0], fx_r.at[d, 0], xdir[d])
        send(fpiece(xnear[d], part(d)), fx_s.at[d, 1], fx_r.at[d, 1], xdir[d])
    vz_wait(1)
    vz_send(2)
    vx_send1(-1)
    vx_send1(1)
    for d in range(2):
        arrived(fpiece(xfar, part(d)), fx_s.at[d, 1], fx_r.at[d, 1], xdir[d])
    fz_send(1)
    vz_wait(2)
    vz_send(3)
    vx_send1(-2)
    vx_send1(2)
    vx_send2(0)
    vz_wait(3)
    vz_send(4)
    vx_send1(-3)
    vx_send1(3)
    fz_step(1)
    vx_send2(-1)
    vx_send2(1)
    vz_wait(4)
    vx_send1(4)
    fz_step(2)
    vx_send2(-2)
    vx_send2(2)

    @pl.when(r > 0)
    def _():
        pltpu.make_async_remote_copy(
            src_ref=x_buf.at[pl.ds(B, B), :], dst_ref=xp_buf, send_sem=xc_s.at[0], recv_sem=xc_r.at[0],
            device_id=(c, r), device_id_type=MESH,
        ).wait_recv()

    for i in range(4):
        rows = pl.ds(256 * i, 256)
        v = x_buf[rows, :].T
        xt[:, rows] = v
        put(xs, (slice(None), pl.ds(B + 256 * i, 256)), v)
    for i in range(2):
        put(xs, (slice(None), pl.ds(256 * i, 256)), xp_buf[pl.ds(256 * i, 256), :].T)

    fz_step(3)
    for dz in (-3, 3, 4):
        vx_send2(dz)
    for dz in (0, -1, 1, -2, 2, -3, 3, 4):
        vx_last(dz)

    has_upper = r > 0
    for vs, i in ((vs1, 0), (vs2, 1)):
        for qq in range(4):
            v = vt_buf[i, pl.ds(2 * qq, 2)].reshape(128, BAND)
            if i == 0:
                v = jnp.where(has_upper, v, jnp.zeros_like(v))
            rows = pl.ds(128 * qq, 128)
            put(vs, (rows, pl.ds(128 * qq, BAND)), v)
            gap = (640, 0, 896, 256)[qq]
            for k in range(2):
                vs[k, rows, pl.ds(gap, 128)] = jnp.zeros((128, 128), BF16)

    for cref, vs, off in ((c1, vs1, 0), (c2, vs2, B)):
        for a in range(2):
            w = pl.ds(256 * a, 768)
            cref[:, pl.ds(256 * a, 256)] = dot3(
                get(xs, slice(None), pl.ds(off + 256 * a, 768)), get(vs, pl.ds(256 * a, 256), w), NT
            )
    put(ws, (slice(None), slice(None)), c1[...])

    fz_step(4)
    for fs, i in ((fs1, 0), (fs2, 1)):
        for a in range(2):
            put(fs, (pl.ds(256 * a, 256), slice(None)), ft_buf[i, pl.ds(4 * a, 4)].reshape(256, B))

    lower_lower(h1, fs1, vs1, B)
    lower_lower(h2, fs2, vs2, B)
    put(g, (T0, T0), dot3(get(h1, T0, T0), get(vs2, T0, T0), NT))
    put(g, (T1, T0), dot3(get(h1, T1, ALL), get(vs2, T0, ALL), NT))
    put(g, (T1, T1), dot3(get(h1, T1, T1), get(vs2, T1, T1), NT))
    lower_lower(m, g, h2)
    put(at, (T0, T0), dot3(get(vs1, T0, T0), get(m, T0, T0), TN))
    put(at, (T1, T0), dot3(get(vs1, ALL, T1), get(m, ALL, T0), TN))
    put(at, (T1, T1), dot3(get(vs1, T1, T1), get(m, T1, T1), TN))
    for k in range(2):
        at[k, T0, T1] = jnp.zeros((256, 256), BF16)
    left, right = times_lower(ws, g)
    put(ds, (slice(None), T0), c2[:, T0] - left)
    put(ds, (slice(None), T1), c2[:, T1] - right)
    left, right = times_lower(ds, h2)
    e[:, T0] = left
    e[:, T1] = right

    def d_copy(i, rr):
        return pltpu.make_async_remote_copy(
            src_ref=do_buf.at[i], dst_ref=d_buf.at[i], send_sem=d_s.at[i], recv_sem=d_r.at[i],
            device_id=(c, rr), device_id_type=MESH,
        )

    for i in reversed(range(STRIPES)):
        @pl.when(r > 0)
        def _(i=i):
            d_copy(i, r).wait_recv()

        stripe, rest = slice(LC * i, LC * (i + 1)), slice(LC * i, B)
        put(ds, (slice(None), stripe), d_buf[i])
        do_buf[i] = e[:, stripe] + dot3(get(ds, slice(None), rest), get(at, rest, stripe))

        @pl.when(r < last)
        def _(i=i):
            d_copy(i, r + 1).start()

    put(ws, (slice(None), T1), c1[:, T1] - dot3(get(ds, slice(None), T1), get(vs1, T1, T1), NT))
    put(ws, (slice(None), T0), c1[:, T0] - dot3(get(ds, slice(None), ALL), get(vs1, T0, ALL), NT))
    left, right = times_lower(ws, fs1)
    put(zs1, (slice(None), T0), left)
    put(zs1, (slice(None), T1), right)

    def ret_copy(i, rr):
        return pltpu.make_async_remote_copy(
            src_ref=ro_buf.at[i], dst_ref=ret_buf.at[i], send_sem=ret_s.at[i], recv_sem=ret_r.at[i],
            device_id=(c, rr), device_id_type=MESH,
        )

    left, right = times_upper(zs1, vs1)
    for i, v in enumerate((left, right)):
        ro_buf[i] = v

        @pl.when(r > 0)
        def _(i=i):
            ret_copy(i, r - 1).start()

    left, right = times_lower(ws, g)
    put(ds, (slice(None), T0), c2[:, T0] - left)
    put(ds, (slice(None), T1), c2[:, T1] - right)
    left, right = times_lower(ds, fs2)
    put(zs2, (slice(None), T0), left)
    put(zs2, (slice(None), T1), right)
    low = times_lower(zs1, vs1, B)
    upp = times_upper(zs2, vs2)
    for i in range(2):
        cols = slice(256 * i, 256 * (i + 1))
        out[pl.ds(256 * i, 256), :] = (xt[:, cols] - low[i] - upp[i]).T

    for i in range(2):
        @pl.when(r < last)
        def _(i=i):
            ret_copy(i, r).wait_recv()

        for j in range(256 // LC):
            k = i * (256 // LC) + j
            lanes_k = slice(B + LC * k, B + LC * (k + 1))
            v = xt[:, lanes_k] - do_buf[k] - ret_buf[i, :, slice(LC * j, LC * (j + 1))]
            out[pl.ds(B + LC * k, LC), :] = v.T

    for cp in sent:
        cp.wait_send()

    @pl.when(r < last)
    def _():
        pltpu.make_async_remote_copy(
            src_ref=x_buf.at[pl.ds(B, B), :], dst_ref=xp_buf, send_sem=xc_s.at[0], recv_sem=xc_r.at[0],
            device_id=(c, r + 1), device_id_type=MESH,
        ).wait_send()
        for i in range(STRIPES):
            d_copy(i, r + 1).wait_send()

    @pl.when(r > 0)
    def _():
        for i in range(2):
            ret_copy(i, r - 1).wait_send()


def body(vectors, reflectors, factors):
    vmem = pltpu.VMEM
    dma = pltpu.SemaphoreType.DMA
    pair = (2, N, B)
    square = (2, B, B)
    scratch = [
        vmem((2, NZ, 64, BAND), F32), vmem((2, NZ, 64, B), F32),
        vmem((2 * B, N), F32), vmem((B, N), F32),
        vmem((STRIPES, N, LC), F32), vmem((STRIPES, N, LC), F32),
        vmem((2, N, HALF), F32), vmem((2, N, HALF), F32),
        vmem((2, N, 3 * B), BF16),
        vmem((2, B, 2 * B), BF16), vmem((2, B, 2 * B), BF16),
        vmem(square, BF16), vmem(square, BF16),
        vmem(square, BF16), vmem(square, BF16), vmem(square, BF16), vmem(square, BF16), vmem(square, BF16),
        vmem(pair, BF16), vmem(pair, BF16), vmem(pair, BF16), vmem(pair, BF16),
        vmem((N, B), F32), vmem((N, B), F32), vmem((N, B), F32), vmem((N, 2 * B), F32),
        dma((5,)), dma((2,)), dma((2,)), dma((2, 4)), dma((2, 4)), dma((2, 2, NZ)), dma((2, 2, NZ)),
        dma((2, 2)), dma((2, 2)), dma((2, 2, 4)), dma((2, 2, 4)),
        dma((1,)), dma((1,)), dma((STRIPES,)), dma((STRIPES,)), dma((2,)), dma((2,)),
    ]
    return pl.pallas_call(
        kernel,
        out_shape=jax.ShapeDtypeStruct((2 * B, N), F32),
        in_specs=[pl.BlockSpec(memory_space=pl.ANY)] * 3,
        out_specs=pl.BlockSpec(memory_space=pltpu.VMEM),
        scratch_shapes=scratch,
        compiler_params=pltpu.CompilerParams(
            collective_id=0, has_side_effects=True, vmem_limit_bytes=56 << 20
        ),
    )(vectors, jnp.transpose(reflectors, (0, 2, 1)), jnp.transpose(factors, (0, 2, 1)))


def solution(mesh):
    placed = (P("rows", "cols"), P(None, None, "cols"), P(None, None, "cols"))
    return jax.shard_map(
        body, mesh=mesh, in_specs=placed, out_specs=P("rows", "cols"), check_vma=False
    )
```

```python
import jax
import jax.numpy as jnp
from jax import lax
from jax.experimental import pallas as pl
from jax.experimental.pallas import tpu as pltpu
from jax.sharding import PartitionSpec as P

MESH = pl.DeviceIdType.MESH
F32, BF16 = jnp.float32, jnp.bfloat16
NZ, NX, NH = 8, 4, 2
B, HALF, N = 512, 256, 256
BAND = 640
LC = 128
STRIPES = B // LC
NN = (((1,), (0,)), ((), ()))
NT = (((1,), (1,)), ((), ()))
TN = (((0,), (0,)), ((), ()))


def split(v):
    hi = v.astype(BF16)
    return hi, (v - hi.astype(F32)).astype(BF16)


def dot3(a, b, dims=NN):
    def one(u, v):
        return lax.dot_general(u, v, dims, preferred_element_type=F32)

    return one(a[0], b[0]) + one(a[0], b[1]) + one(a[1], b[0])


def put(ref, at, v):
    hi, lo = split(v)
    ref[(0, *at)] = hi
    ref[(1, *at)] = lo


def get(ref, rows, cols):
    return ref[0, rows, cols], ref[1, rows, cols]


ALL, T0, T1 = slice(0, 512), slice(0, 256), slice(256, 512)


def times_lower(a, m, off=0):
    lo, hi = slice(off, off + 256), slice(off + 256, off + 512)
    left = dot3(get(a, slice(None), ALL), get(m, ALL, lo))
    right = dot3(get(a, slice(None), T1), get(m, T1, hi))
    return left, right


def times_upper(a, m):
    left = dot3(get(a, slice(None), T0), get(m, T0, T0))
    right = dot3(get(a, slice(None), ALL), get(m, ALL, T1))
    return left, right


def lower_lower(out, a, m, off=0):
    lo, hi = slice(off, off + 256), slice(off + 256, off + 512)
    put(out, (T0, T0), dot3(get(a, T0, T0), get(m, T0, lo)))
    put(out, (T1, T0), dot3(get(a, T1, ALL), get(m, ALL, lo)))
    put(out, (T1, T1), dot3(get(a, T1, T1), get(m, T1, hi)))


def kernel(
    vec, rft, fat, out,
    vt_buf, ft_buf, x_buf, xp_buf, d_buf, do_buf, ret_buf, ro_buf,
    xs, vs1, vs2, fs1, fs2, h1, h2, g, m, at, ds, ws, zs1, zs2,
    c1, c2, e, xt,
    lsem, p_s, p_r, vz_s, vz_r, vx_s, vx_r, wx_s, wx_r, wz_s, wz_r, fx_s, fx_r, fz_s, fz_r,
    xc_s, xc_r, d_s, d_r, ret_s, ret_r,
):
    c = lax.axis_index("cols")
    r = lax.axis_index("rows")
    z, x, h = c // (NX * NH), (c // NH) % NX, c % NH
    q = z // 2
    last = lax.axis_size("rows") - 1

    def at_c(zz, xx, hh):
        return (zz * NX + xx) * NH + hh

    zp, zm = at_c((z + 1) % NZ, x, h), at_c((z + NZ - 1) % NZ, x, h)
    xp, xm = at_c(z, (x + 1) % NX, h), at_c(z, (x + NX - 1) % NX, h)
    twin = at_c(z, x, 1 - h)
    b_first, b_own = jnp.maximum(2 * r - 1, 0), 2 * r
    zdir, xdir = (zp, zm), (xp, xm)

    lanes = pl.ds(pl.multiple_of(128 * q, 128), BAND)
    local = []
    for i, b in enumerate((b_first, b_own)):
        local.append(pltpu.make_async_copy(rft.at[b, :, lanes], vt_buf.at[i, z, x, h], lsem.at[2 * i]))
        local.append(pltpu.make_async_copy(fat.at[b], ft_buf.at[i, z, x, h], lsem.at[2 * i + 1]))
    xload = pltpu.make_async_copy(vec, x_buf, lsem.at[4])
    for cp in local:
        cp.start()
    xload.start()

    barrier = pltpu.get_barrier_semaphore()
    for cc in (zp, zm, xp, xm, twin):
        pl.semaphore_signal(barrier, inc=1, device_id=(cc, r), device_id_type=MESH)

    @pl.when(r > 0)
    def _():
        pl.semaphore_signal(barrier, inc=1, device_id=(c, r - 1), device_id_type=MESH)

    @pl.when(r < last)
    def _():
        pl.semaphore_signal(barrier, inc=1, device_id=(c, r + 1), device_id_type=MESH)

    @pl.when(r == 0)
    def _():
        xp_buf[...] = jnp.zeros_like(xp_buf)
        d_buf[...] = jnp.zeros_like(d_buf)

    @pl.when(r == last)
    def _():
        ret_buf[...] = jnp.zeros_like(ret_buf)

    for i in range(2):
        vs = (vs1, vs2)[i]
        for qq in range(4):
            gap = (640, 0, 896, 256)[qq]
            for k in range(2):
                vs[k, pl.ds(128 * qq, 128), pl.ds(gap, 128)] = jnp.zeros((128, 128), BF16)
    for ref in (fs1, fs2):
        for k in range(2):
            ref[k, pl.ds(0, 128), pl.ds(128, 128)] = jnp.zeros((128, 128), BF16)
            ref[k, pl.ds(256, 128), pl.ds(384, 128)] = jnp.zeros((128, 128), BF16)
    for cp in local:
        cp.wait()
    xload.wait()
    for i in range(4):
        rows = pl.ds(256 * i, 256)
        v = x_buf[rows, :].T
        xt[:, rows] = v
        put(xs, (slice(None), pl.ds(B + 256 * i, 256)), v)

    pl.semaphore_wait(barrier, 5 + jnp.minimum(r, 1) + jnp.minimum(last - r, 1))

    sent = []

    def remote(ref, ssem, rsem, cc):
        return pltpu.make_async_remote_copy(
            src_ref=ref, dst_ref=ref, send_sem=ssem, recv_sem=rsem,
            device_id=(cc, r), device_id_type=MESH,
        )

    def send(ref, ssem, rsem, cc):
        cp = remote(ref, ssem, rsem, cc)
        cp.start()
        sent.append(cp.wait_send)

    def arrived(ref, ssem, rsem, cc):
        remote(ref, ssem, rsem, cc).wait_recv()

    def by_width(zz, do):
        for w in range(4):
            @pl.when(zz // 2 == w)
            def _(w=w):
                do(128 * (w + 1))

    def slab(dz):
        return (z + dz + NZ) % NZ

    both = slice(None)
    xnear = ((x + NX - 1) % NX, (x + 1) % NX)
    xfar = (x + 2) % NX

    def part(d):
        return pl.ds(d, 1)

    def vz_args(n, d, dz):
        half = both if n < 4 else part(d)
        return vt_buf.at[0, slab(dz), x, half], vz_s.at[d, n - 1], vz_r.at[d, n - 1], zdir[d]

    def vz_send(n):
        for d in range(2):
            send(*vz_args(n, d, (1 - n) if d == 0 else (n - 1)))

    def vz_step(n):
        for d in range(2):
            arrived(*vz_args(n, d, -n if d == 0 else n))
            if n < 4:
                send(*vz_args(n + 1, d, -n if d == 0 else n))

    def vx_args(dz, n, d, xx):
        half = both if n == 0 else part(d)
        k = dz % NZ
        return vt_buf.at[0, slab(dz), xx, half], vx_s.at[d, n, k], vx_r.at[d, n, k], xdir[d]

    def wx_args(n, d, xx):
        half = both if n == 0 else part(d)
        return vt_buf.at[1, z, xx, half], wx_s.at[d, n], wx_r.at[d, n], xdir[d]

    def wz_args(n, d, p, dz):
        return vt_buf.at[1, slab(dz), pl.ds(2 * p, 2)], wz_s.at[d, p, n - 1], wz_r.at[d, p, n - 1], zdir[d]

    def wz_step(n):
        for p in range(2):
            for d in range(2):
                if n == 4 and p != d:
                    continue
                dz = -n if d == 0 else n
                if n > 0:
                    arrived(*wz_args(n, d, p, dz))
                if n < 3 or (n == 3 and p == d):
                    send(*wz_args(n + 1, d, p, dz))

    def fz_args(n, d, dz):
        blk = both if n < 4 else part(d)
        return ft_buf.at[blk, slab(dz), x], fz_s.at[d, n - 1], fz_r.at[d, n - 1], zdir[d]

    def fz_send(n):
        for d in range(2):
            send(*fz_args(n, d, (1 - n) if d == 0 else (n - 1)))

    def fz_step(n):
        for d in range(2):
            arrived(*fz_args(n, d, -n if d == 0 else n))
            if n < 4:
                send(*fz_args(n + 1, d, -n if d == 0 else n))

    def fx(dz, n, d, xx, do):
        blk, k = both if n == 0 else part(d), dz % NZ

        def at_width(width):
            do(remote(
                ft_buf.at[blk, slab(dz), xx, :, :, pl.ds(0, width)],
                fx_s.at[d, n, k], fx_r.at[d, n, k], xdir[d],
            ))

        by_width(slab(dz), at_width)

    def fx_go(dz, n, d, xx):
        fx(dz, n, d, xx, lambda cp: cp.start())
        sent.append(lambda: fx(dz, n, d, xx, lambda cp: cp.wait_send()))

    def x_send1(*dzs):
        for dz in dzs:
            for d in range(2):
                send(*vx_args(dz, 0, d, x))

    def fx_send1(*dzs):
        for dz in dzs:
            for d in range(2):
                fx_go(dz, 0, d, x)

    def x_send2(*dzs):
        for dz in dzs:
            for d in range(2):
                arrived(*vx_args(dz, 0, d, xnear[d]))
                send(*vx_args(dz, 1, d, xnear[d]))

    def fx_send2(*dzs):
        for dz in dzs:
            for d in range(2):
                fx(dz, 0, d, xnear[d], lambda cp: cp.wait_recv())
                fx_go(dz, 1, d, xnear[d])

    def x_last(*dzs):
        for dz in dzs:
            for d in range(2):
                arrived(*vx_args(dz, 1, d, xfar))

    def fx_last(*dzs):
        for dz in dzs:
            for d in range(2):
                fx(dz, 1, d, xfar, lambda cp: cp.wait_recv())

    def twin_args(ref, k, hh):
        return ref.at[both, z, x, hh], p_s.at[k], p_r.at[k], twin

    send(*twin_args(vt_buf, 0, h))
    send(*twin_args(ft_buf, 1, h))
    arrived(*twin_args(vt_buf, 0, 1 - h))
    for d in range(2):
        send(*wx_args(0, d, x))
    vz_send(1)
    arrived(*twin_args(ft_buf, 1, 1 - h))
    fz_send(1)
    x_send1(0)
    fx_send1(0)

    @pl.when(r < last)
    def _():
        pltpu.make_async_remote_copy(
            src_ref=x_buf.at[pl.ds(B, B), :], dst_ref=xp_buf, send_sem=xc_s.at[0], recv_sem=xc_r.at[0],
            device_id=(c, r + 1), device_id_type=MESH,
        ).start()

    for d in range(2):
        arrived(*wx_args(0, d, xnear[d]))
        send(*wx_args(1, d, xnear[d]))
    vz_step(1)
    fz_step(1)
    x_send1(-1, 1)
    fx_send1(-1, 1)
    for d in range(2):
        arrived(*wx_args(1, d, xfar))
    wz_step(0)
    vz_step(2)
    fz_step(2)
    x_send1(-2, 2)
    fx_send1(-2, 2)
    x_send2(0)
    fx_send2(0)
    wz_step(1)
    vz_step(3)
    fz_step(3)
    x_send1(-3, 3)
    fx_send1(-3, 3)
    x_send2(-1, 1)
    fx_send2(-1, 1)
    vz_step(4)
    fz_step(4)
    x_send1(4)
    fx_send1(4)
    wz_step(2)
    x_send2(-2, 2)
    fx_send2(-2, 2)
    wz_step(3)
    x_send2(-3, 3, 4)
    fx_send2(-3, 3, 4)

    @pl.when(r > 0)
    def _():
        pltpu.make_async_remote_copy(
            src_ref=x_buf.at[pl.ds(B, B), :], dst_ref=xp_buf, send_sem=xc_s.at[0], recv_sem=xc_r.at[0],
            device_id=(c, r), device_id_type=MESH,
        ).wait_recv()

    for i in range(2):
        put(xs, (slice(None), pl.ds(256 * i, 256)), xp_buf[pl.ds(256 * i, 256), :].T)
    wz_step(4)
    x_last(0, -1, 1, -2, 2, -3, 3, 4)

    has_upper = r > 0
    for vs, i in ((vs1, 0), (vs2, 1)):
        for qq in range(4):
            v = vt_buf[i, pl.ds(2 * qq, 2)].reshape(128, BAND)
            if i == 0:
                v = jnp.where(has_upper, v, jnp.zeros_like(v))
            rows = pl.ds(128 * qq, 128)
            put(vs, (rows, pl.ds(128 * qq, BAND)), v)

    for cref, vs, off in ((c1, vs1, 0), (c2, vs2, B)):
        for a in range(2):
            w = pl.ds(256 * a, 768)
            cref[:, pl.ds(256 * a, 256)] = dot3(
                get(xs, slice(None), pl.ds(off + 256 * a, 768)), get(vs, pl.ds(256 * a, 256), w), NT
            )
    put(ws, (slice(None), slice(None)), c1[...])

    fx_last(0, -1, 1, -2, 2, -3, 3, 4)
    for fs, i in ((fs1, 0), (fs2, 1)):
        for qq in range(4):
            w = pl.ds(0, 128 * (qq + 1))
            v = ft_buf[i, pl.ds(2 * qq, 2), :, :, :, w].reshape(128, 128 * (qq + 1))
            put(fs, (pl.ds(128 * qq, 128), w), v)

    lower_lower(h1, fs1, vs1, B)
    lower_lower(h2, fs2, vs2, B)
    put(g, (T0, T0), dot3(get(h1, T0, T0), get(vs2, T0, T0), NT))
    put(g, (T1, T0), dot3(get(h1, T1, ALL), get(vs2, T0, ALL), NT))
    put(g, (T1, T1), dot3(get(h1, T1, T1), get(vs2, T1, T1), NT))
    lower_lower(m, g, h2)
    put(at, (T0, T0), dot3(get(vs1, T0, T0), get(m, T0, T0), TN))
    put(at, (T1, T0), dot3(get(vs1, ALL, T1), get(m, ALL, T0), TN))
    put(at, (T1, T1), dot3(get(vs1, T1, T1), get(m, T1, T1), TN))
    for k in range(2):
        at[k, T0, T1] = jnp.zeros((256, 256), BF16)
    left, right = times_lower(ws, g)
    put(ds, (slice(None), T0), c2[:, T0] - left)
    put(ds, (slice(None), T1), c2[:, T1] - right)
    left, right = times_lower(ds, h2)
    e[:, T0] = left
    e[:, T1] = right

    def d_copy(i, rr):
        return pltpu.make_async_remote_copy(
            src_ref=do_buf.at[i], dst_ref=d_buf.at[i], send_sem=d_s.at[i], recv_sem=d_r.at[i],
            device_id=(c, rr), device_id_type=MESH,
        )

    for i in reversed(range(STRIPES)):
        @pl.when(r > 0)
        def _(i=i):
            d_copy(i, r).wait_recv()

        stripe, rest = slice(LC * i, LC * (i + 1)), slice(LC * i, B)
        put(ds, (slice(None), stripe), d_buf[i])
        do_buf[i] = e[:, stripe] + dot3(get(ds, slice(None), rest), get(at, rest, stripe))

        @pl.when(r < last)
        def _(i=i):
            d_copy(i, r + 1).start()

    put(ws, (slice(None), T1), c1[:, T1] - dot3(get(ds, slice(None), T1), get(vs1, T1, T1), NT))
    put(ws, (slice(None), T0), c1[:, T0] - dot3(get(ds, slice(None), ALL), get(vs1, T0, ALL), NT))
    left, right = times_lower(ws, fs1)
    put(zs1, (slice(None), T0), left)
    put(zs1, (slice(None), T1), right)

    def ret_copy(i, rr):
        return pltpu.make_async_remote_copy(
            src_ref=ro_buf.at[i], dst_ref=ret_buf.at[i], send_sem=ret_s.at[i], recv_sem=ret_r.at[i],
            device_id=(c, rr), device_id_type=MESH,
        )

    left, right = times_upper(zs1, vs1)
    for i, v in enumerate((left, right)):
        ro_buf[i] = v

        @pl.when(r > 0)
        def _(i=i):
            ret_copy(i, r - 1).start()

    left, right = times_lower(ws, g)
    put(ds, (slice(None), T0), c2[:, T0] - left)
    put(ds, (slice(None), T1), c2[:, T1] - right)
    left, right = times_lower(ds, fs2)
    put(zs2, (slice(None), T0), left)
    put(zs2, (slice(None), T1), right)
    low = times_lower(zs1, vs1, B)
    upp = times_upper(zs2, vs2)
    for i in range(2):
        cols = slice(256 * i, 256 * (i + 1))
        out[pl.ds(256 * i, 256), :] = (xt[:, cols] - low[i] - upp[i]).T

    for i in range(2):
        @pl.when(r < last)
        def _(i=i):
            ret_copy(i, r).wait_recv()

        for j in range(256 // LC):
            k = i * (256 // LC) + j
            lanes_k = slice(B + LC * k, B + LC * (k + 1))
            v = xt[:, lanes_k] - do_buf[k] - ret_buf[i, :, slice(LC * j, LC * (j + 1))]
            out[pl.ds(B + LC * k, LC), :] = v.T

    for done in sent:
        done()

    @pl.when(r < last)
    def _():
        pltpu.make_async_remote_copy(
            src_ref=x_buf.at[pl.ds(B, B), :], dst_ref=xp_buf, send_sem=xc_s.at[0], recv_sem=xc_r.at[0],
            device_id=(c, r + 1), device_id_type=MESH,
        ).wait_send()
        for i in range(STRIPES):
            d_copy(i, r + 1).wait_send()

    @pl.when(r > 0)
    def _():
        for i in range(2):
            ret_copy(i, r - 1).wait_send()


def body(vectors, reflectors, factors):
    vmem = pltpu.VMEM
    dma = pltpu.SemaphoreType.DMA
    pair = (2, N, B)
    square = (2, B, B)
    scratch = [
        vmem((2, NZ, NX, NH, 8, BAND), F32), vmem((2, NZ, NX, NH, 8, B), F32),
        vmem((2 * B, N), F32), vmem((B, N), F32),
        vmem((STRIPES, N, LC), F32), vmem((STRIPES, N, LC), F32),
        vmem((2, N, HALF), F32), vmem((2, N, HALF), F32),
        vmem((2, N, 3 * B), BF16),
        vmem((2, B, 2 * B), BF16), vmem((2, B, 2 * B), BF16),
        vmem(square, BF16), vmem(square, BF16),
        vmem(square, BF16), vmem(square, BF16), vmem(square, BF16), vmem(square, BF16), vmem(square, BF16),
        vmem(pair, BF16), vmem(pair, BF16), vmem(pair, BF16), vmem(pair, BF16),
        vmem((N, B), F32), vmem((N, B), F32), vmem((N, B), F32), vmem((N, 2 * B), F32),
        dma((5,)), dma((2,)), dma((2,)), dma((2, 4)), dma((2, 4)), dma((2, 2, NZ)), dma((2, 2, NZ)),
        dma((2, 2)), dma((2, 2)), dma((2, 2, 4)), dma((2, 2, 4)),
        dma((2, 2, NZ)), dma((2, 2, NZ)), dma((2, 4)), dma((2, 4)),
        dma((1,)), dma((1,)), dma((STRIPES,)), dma((STRIPES,)), dma((2,)), dma((2,)),
    ]
    return pl.pallas_call(
        kernel,
        out_shape=jax.ShapeDtypeStruct((2 * B, N), F32),
        in_specs=[pl.BlockSpec(memory_space=pl.ANY)] * 3,
        out_specs=pl.BlockSpec(memory_space=pltpu.VMEM),
        scratch_shapes=scratch,
        compiler_params=pltpu.CompilerParams(
            collective_id=0, has_side_effects=True, vmem_limit_bytes=56 << 20
        ),
    )(vectors, jnp.transpose(reflectors, (0, 2, 1)), jnp.transpose(factors, (0, 2, 1)))


def solution(mesh):
    placed = (P("rows", "cols"), P(None, None, "cols"), P(None, None, "cols"))
    return jax.shard_map(
        body, mesh=mesh, in_specs=placed, out_specs=P("rows", "cols"), check_vma=False
    )
```

```python
import jax
import jax.numpy as jnp
from jax import lax
from jax.experimental import pallas as pl
from jax.experimental.pallas import tpu as pltpu
from jax.sharding import PartitionSpec as P

MESH = pl.DeviceIdType.MESH
F32, BF16 = jnp.float32, jnp.bfloat16
NZ, NX, NH = 8, 4, 2
B, HALF, N = 512, 256, 256
BAND = 640
LC = 128
STRIPES = B // LC
PARTS = 2
NC = N // PARTS
NN = (((1,), (0,)), ((), ()))
NT = (((1,), (1,)), ((), ()))
TN = (((0,), (0,)), ((), ()))


def split(v):
    hi = v.astype(BF16)
    return hi, (v - hi.astype(F32)).astype(BF16)


def dot3(a, b, dims=NN):
    def one(u, v):
        return lax.dot_general(u, v, dims, preferred_element_type=F32)

    return one(a[0], b[0]) + one(a[0], b[1]) + one(a[1], b[0])


def put(ref, at, v):
    hi, lo = split(v)
    ref[(0, *at)] = hi
    ref[(1, *at)] = lo


def get(ref, rows, cols):
    return ref[0, rows, cols], ref[1, rows, cols]


ALL, T0, T1 = slice(0, 512), slice(0, 256), slice(256, 512)


def times_lower(a, m, off=0, rows=slice(None)):
    lo, hi = slice(off, off + 256), slice(off + 256, off + 512)
    left = dot3(get(a, rows, ALL), get(m, ALL, lo))
    right = dot3(get(a, rows, T1), get(m, T1, hi))
    return left, right


def times_upper(a, m, rows):
    left = dot3(get(a, rows, T0), get(m, T0, T0))
    right = dot3(get(a, rows, ALL), get(m, ALL, T1))
    return left, right


def lower_lower(out, a, m, off=0):
    lo, hi = slice(off, off + 256), slice(off + 256, off + 512)
    put(out, (T0, T0), dot3(get(a, T0, T0), get(m, T0, lo)))
    put(out, (T1, T0), dot3(get(a, T1, ALL), get(m, ALL, lo)))
    put(out, (T1, T1), dot3(get(a, T1, T1), get(m, T1, hi)))


def kernel(
    vec, rft, fat, out,
    vt_buf, ft_buf, x_buf, xp_buf, d_buf, do_buf, ret_buf, ro_buf,
    xs, vs1, vs2, fs1, fs2, h1, h2, g, m, at, ds, ws, zs1, zs2,
    c1, c2, e, xt,
    gv_buf, gf_buf, gsem, lsem, p_s, p_r, vz_s, vz_r, vx_s, vx_r, wx_s, wx_r, wz_s, wz_r, fx_s, fx_r, fz_s, fz_r,
    xc_s, xc_r, d_s, d_r, ret_s, ret_r,
):
    c = lax.axis_index("cols")
    r = lax.axis_index("rows")
    z, x, h = c // (NX * NH), (c // NH) % NX, c % NH
    q = z // 2
    last = lax.axis_size("rows") - 1

    def at_c(zz, xx, hh):
        return (zz * NX + xx) * NH + hh

    zp, zm = at_c((z + 1) % NZ, x, h), at_c((z + NZ - 1) % NZ, x, h)
    xp, xm = at_c(z, (x + 1) % NX, h), at_c(z, (x + NX - 1) % NX, h)
    twin = at_c(z, x, 1 - h)
    b_first, b_own = jnp.maximum(2 * r - 1, 0), 2 * r
    zdir, xdir = (zp, zm), (xp, xm)

    lanes = pl.ds(pl.multiple_of(128 * q, 128), BAND)
    local = []
    for i, b in enumerate((b_first, b_own)):
        local.append(pltpu.make_async_copy(rft.at[b, :, lanes], vt_buf.at[i, z, x, h], lsem.at[2 * i]))
        local.append(pltpu.make_async_copy(fat.at[b], ft_buf.at[i, z, x, h], lsem.at[2 * i + 1]))
    xload = pltpu.make_async_copy(vec, x_buf, lsem.at[4])
    for cp in local:
        cp.start()
    xload.start()

    y, core = r // 2, r % 2
    near = 2 * jnp.where(y < 2, 3, 0) + core
    giver = (y == 0) | (y == 3)
    takers = [2 * (jnp.where(y == 3, 0, 2) + t) + core for t in range(2)]

    def gift(t, i):
        b = 2 * takers[t] if i else jnp.maximum(2 * takers[t] - 1, 0)
        return (
            pltpu.make_async_copy(rft.at[b, :, lanes], gv_buf.at[t, i], gsem.at[t, i, 0]),
            pltpu.make_async_copy(fat.at[b], gf_buf.at[t, i], gsem.at[t, i, 1]),
        )

    def given(t, k):
        src, dst = (gv_buf, vt_buf) if k == 0 else (gf_buf, ft_buf)
        return pltpu.make_async_remote_copy(
            src_ref=src.at[t], dst_ref=dst.at[:, z, x, h], send_sem=p_s.at[t, k], recv_sem=p_r.at[k],
            device_id=(twin, takers[t]), device_id_type=MESH,
        )

    @pl.when(giver)
    def _():
        for t in range(2):
            for i in range(2):
                for cp in gift(t, i):
                    cp.start()

    barrier = pltpu.get_barrier_semaphore()
    for cc in (zp, zm, xp, xm):
        pl.semaphore_signal(barrier, inc=1, device_id=(cc, r), device_id_type=MESH)

    pl.semaphore_signal(barrier, inc=1, device_id=(twin, near), device_id_type=MESH)

    @pl.when(giver)
    def _():
        for t in range(2):
            pl.semaphore_signal(barrier, inc=1, device_id=(twin, takers[t]), device_id_type=MESH)

    @pl.when(r > 0)
    def _():
        pl.semaphore_signal(barrier, inc=1, device_id=(c, r - 1), device_id_type=MESH)

    @pl.when(r < last)
    def _():
        pl.semaphore_signal(barrier, inc=1, device_id=(c, r + 1), device_id_type=MESH)

    @pl.when(r == 0)
    def _():
        xp_buf[...] = jnp.zeros_like(xp_buf)
        d_buf[...] = jnp.zeros_like(d_buf)

    @pl.when(r == last)
    def _():
        ret_buf[...] = jnp.zeros_like(ret_buf)

    for i in range(2):
        vs = (vs1, vs2)[i]
        for qq in range(4):
            gap = (640, 0, 896, 256)[qq]
            for k in range(2):
                vs[k, pl.ds(128 * qq, 128), pl.ds(gap, 128)] = jnp.zeros((128, 128), BF16)
    for ref in (fs1, fs2):
        for k in range(2):
            ref[k, pl.ds(0, 128), pl.ds(128, 128)] = jnp.zeros((128, 128), BF16)
            ref[k, pl.ds(256, 128), pl.ds(384, 128)] = jnp.zeros((128, 128), BF16)
    for cp in local:
        cp.wait()
    xload.wait()
    for i in range(4):
        rows = pl.ds(256 * i, 256)
        v = x_buf[rows, :].T
        xt[:, rows] = v
        put(xs, (slice(None), pl.ds(B + 256 * i, 256)), v)

    @pl.when(giver)
    def _():
        for t in range(2):
            for i in range(2):
                for cp in gift(t, i):
                    cp.wait()

    peers = 5 + jnp.minimum(r, 1) + jnp.minimum(last - r, 1) + jnp.where(giver, 2, 0)
    pl.semaphore_wait(barrier, peers)

    @pl.when(giver)
    def _():
        for k in range(2):
            for t in range(2):
                given(t, k).start()

    sent = []

    def remote(ref, ssem, rsem, cc):
        return pltpu.make_async_remote_copy(
            src_ref=ref, dst_ref=ref, send_sem=ssem, recv_sem=rsem,
            device_id=(cc, r), device_id_type=MESH,
        )

    def send(ref, ssem, rsem, cc):
        cp = remote(ref, ssem, rsem, cc)
        cp.start()
        sent.append(cp.wait_send)

    def arrived(ref, ssem, rsem, cc):
        remote(ref, ssem, rsem, cc).wait_recv()

    def by_width(zz, do):
        for w in range(4):
            @pl.when(zz // 2 == w)
            def _(w=w):
                do(128 * (w + 1))

    def slab(dz):
        return (z + dz + NZ) % NZ

    both = slice(None)
    xnear = ((x + NX - 1) % NX, (x + 1) % NX)
    xfar = (x + 2) % NX

    def part(d):
        return pl.ds(d, 1)

    def vz_args(n, d, dz):
        half = both if n < 4 else part(d)
        return vt_buf.at[0, slab(dz), x, half], vz_s.at[d, n - 1], vz_r.at[d, n - 1], zdir[d]

    def vz_send(n):
        for d in range(2):
            send(*vz_args(n, d, (1 - n) if d == 0 else (n - 1)))

    def vz_step(n):
        for d in range(2):
            arrived(*vz_args(n, d, -n if d == 0 else n))
            if n < 4:
                send(*vz_args(n + 1, d, -n if d == 0 else n))

    def vx_args(dz, n, d, xx):
        half = both if n == 0 else part(d)
        k = dz % NZ
        return vt_buf.at[0, slab(dz), xx, half], vx_s.at[d, n, k], vx_r.at[d, n, k], xdir[d]

    def wx_args(n, d, xx):
        half = both if n == 0 else part(d)
        return vt_buf.at[1, z, xx, half], wx_s.at[d, n], wx_r.at[d, n], xdir[d]

    def wz_args(n, d, p, dz):
        return vt_buf.at[1, slab(dz), pl.ds(2 * p, 2)], wz_s.at[d, p, n - 1], wz_r.at[d, p, n - 1], zdir[d]

    def wz_step(n):
        for p in range(2):
            for d in range(2):
                if n == 4 and p != d:
                    continue
                dz = -n if d == 0 else n
                if n > 0:
                    arrived(*wz_args(n, d, p, dz))
                if n < 3 or (n == 3 and p == d):
                    send(*wz_args(n + 1, d, p, dz))

    def fz_args(n, d, dz):
        blk = both if n < 4 else part(d)
        return ft_buf.at[blk, slab(dz), x], fz_s.at[d, n - 1], fz_r.at[d, n - 1], zdir[d]

    def fz_send(n):
        for d in range(2):
            send(*fz_args(n, d, (1 - n) if d == 0 else (n - 1)))

    def fz_step(n):
        for d in range(2):
            arrived(*fz_args(n, d, -n if d == 0 else n))
            if n < 4:
                send(*fz_args(n + 1, d, -n if d == 0 else n))

    def fx(dz, n, d, xx, do):
        blk, k = both if n == 0 else part(d), dz % NZ

        def at_width(width):
            do(remote(
                ft_buf.at[blk, slab(dz), xx, :, :, pl.ds(0, width)],
                fx_s.at[d, n, k], fx_r.at[d, n, k], xdir[d],
            ))

        by_width(slab(dz), at_width)

    def fx_go(dz, n, d, xx):
        fx(dz, n, d, xx, lambda cp: cp.start())
        sent.append(lambda: fx(dz, n, d, xx, lambda cp: cp.wait_send()))

    def x_send1(*dzs):
        for dz in dzs:
            for d in range(2):
                send(*vx_args(dz, 0, d, x))

    def fx_send1(*dzs):
        for dz in dzs:
            for d in range(2):
                fx_go(dz, 0, d, x)

    def x_send2(*dzs):
        for dz in dzs:
            for d in range(2):
                arrived(*vx_args(dz, 0, d, xnear[d]))
                send(*vx_args(dz, 1, d, xnear[d]))

    def fx_send2(*dzs):
        for dz in dzs:
            for d in range(2):
                fx(dz, 0, d, xnear[d], lambda cp: cp.wait_recv())
                fx_go(dz, 1, d, xnear[d])

    def x_last(*dzs):
        for dz in dzs:
            for d in range(2):
                arrived(*vx_args(dz, 1, d, xfar))

    def fx_last(*dzs):
        for dz in dzs:
            for d in range(2):
                fx(dz, 1, d, xfar, lambda cp: cp.wait_recv())

    arrived(vt_buf.at[:, z, x, 1 - h], p_s.at[0, 0], p_r.at[0], twin)
    for d in range(2):
        send(*wx_args(0, d, x))
    vz_send(1)
    arrived(ft_buf.at[:, z, x, 1 - h], p_s.at[0, 1], p_r.at[1], twin)
    fz_send(1)
    x_send1(0)
    fx_send1(0)

    @pl.when(r < last)
    def _():
        pltpu.make_async_remote_copy(
            src_ref=x_buf.at[pl.ds(B, B), :], dst_ref=xp_buf, send_sem=xc_s.at[0], recv_sem=xc_r.at[0],
            device_id=(c, r + 1), device_id_type=MESH,
        ).start()

    for d in range(2):
        arrived(*wx_args(0, d, xnear[d]))
        send(*wx_args(1, d, xnear[d]))
    vz_step(1)
    fz_step(1)
    x_send1(-1, 1)
    fx_send1(-1, 1)
    for d in range(2):
        arrived(*wx_args(1, d, xfar))
    wz_step(0)
    vz_step(2)
    fz_step(2)
    x_send1(-2, 2)
    fx_send1(-2, 2)
    x_send2(0)
    fx_send2(0)
    wz_step(1)
    vz_step(3)
    fz_step(3)
    x_send1(-3, 3)
    fx_send1(-3, 3)
    x_send2(-1, 1)
    fx_send2(-1, 1)
    vz_step(4)
    fz_step(4)
    x_send1(4)
    fx_send1(4)
    wz_step(2)
    x_send2(-2, 2)
    fx_send2(-2, 2)
    wz_step(3)
    x_send2(-3, 3, 4)
    fx_send2(-3, 3, 4)

    @pl.when(r > 0)
    def _():
        pltpu.make_async_remote_copy(
            src_ref=x_buf.at[pl.ds(B, B), :], dst_ref=xp_buf, send_sem=xc_s.at[0], recv_sem=xc_r.at[0],
            device_id=(c, r), device_id_type=MESH,
        ).wait_recv()

    for i in range(2):
        put(xs, (slice(None), pl.ds(256 * i, 256)), xp_buf[pl.ds(256 * i, 256), :].T)
    wz_step(4)
    x_last(0, -1, 1, -2, 2, -3, 3, 4)

    has_upper = r > 0
    for vs, i in ((vs1, 0), (vs2, 1)):
        for qq in range(4):
            v = vt_buf[i, pl.ds(2 * qq, 2)].reshape(128, BAND)
            if i == 0:
                v = jnp.where(has_upper, v, jnp.zeros_like(v))
            rows = pl.ds(128 * qq, 128)
            put(vs, (rows, pl.ds(128 * qq, BAND)), v)

    for cref, vs, off in ((c1, vs1, 0), (c2, vs2, B)):
        for a in range(2):
            w = pl.ds(256 * a, 768)
            cref[:, pl.ds(256 * a, 256)] = dot3(
                get(xs, slice(None), pl.ds(off + 256 * a, 768)), get(vs, pl.ds(256 * a, 256), w), NT
            )
    put(ws, (slice(None), slice(None)), c1[...])

    fx_last(0, -1, 1, -2, 2, -3, 3, 4)
    for fs, i in ((fs1, 0), (fs2, 1)):
        for qq in range(4):
            w = pl.ds(0, 128 * (qq + 1))
            v = ft_buf[i, pl.ds(2 * qq, 2), :, :, :, w].reshape(128, 128 * (qq + 1))
            put(fs, (pl.ds(128 * qq, 128), w), v)

    lower_lower(h1, fs1, vs1, B)
    lower_lower(h2, fs2, vs2, B)
    put(g, (T0, T0), dot3(get(h1, T0, T0), get(vs2, T0, T0), NT))
    put(g, (T1, T0), dot3(get(h1, T1, ALL), get(vs2, T0, ALL), NT))
    put(g, (T1, T1), dot3(get(h1, T1, T1), get(vs2, T1, T1), NT))
    lower_lower(m, g, h2)
    put(at, (T0, T0), dot3(get(vs1, T0, T0), get(m, T0, T0), TN))
    put(at, (T1, T0), dot3(get(vs1, ALL, T1), get(m, ALL, T0), TN))
    put(at, (T1, T1), dot3(get(vs1, T1, T1), get(m, T1, T1), TN))
    for k in range(2):
        at[k, T0, T1] = jnp.zeros((256, 256), BF16)
    left, right = times_lower(ws, g)
    put(ds, (slice(None), T0), c2[:, T0] - left)
    put(ds, (slice(None), T1), c2[:, T1] - right)
    left, right = times_lower(ds, h2)
    e[:, T0] = left
    e[:, T1] = right

    def d_copy(j, i, rr):
        return pltpu.make_async_remote_copy(
            src_ref=do_buf.at[j, i], dst_ref=d_buf.at[j, i], send_sem=d_s.at[j, i], recv_sem=d_r.at[j, i],
            device_id=(c, rr), device_id_type=MESH,
        )

    def ret_copy(j, rr):
        return pltpu.make_async_remote_copy(
            src_ref=ro_buf.at[j], dst_ref=ret_buf.at[j], send_sem=ret_s.at[j], recv_sem=ret_r.at[j],
            device_id=(c, rr), device_id_type=MESH,
        )

    for j in range(PARTS):
        rows = slice(NC * j, NC * (j + 1))
        for i in reversed(range(STRIPES)):
            @pl.when(r > 0)
            def _(i=i):
                d_copy(j, i, r).wait_recv()

            stripe, rest = slice(LC * i, LC * (i + 1)), slice(LC * i, B)
            put(ds, (rows, stripe), d_buf[j, i])
            do_buf[j, i] = e[rows, stripe] + dot3(get(ds, rows, rest), get(at, rest, stripe))

            @pl.when(r < last)
            def _(i=i):
                d_copy(j, i, r + 1).start()

        put(ws, (rows, T1), c1[rows, T1] - dot3(get(ds, rows, T1), get(vs1, T1, T1), NT))
        put(ws, (rows, T0), c1[rows, T0] - dot3(get(ds, rows, ALL), get(vs1, T0, ALL), NT))
        left, right = times_lower(ws, fs1, 0, rows)
        put(zs1, (rows, T0), left)
        put(zs1, (rows, T1), right)
        left, right = times_upper(zs1, vs1, rows)
        ro_buf[j, :, T0] = left
        ro_buf[j, :, T1] = right

        @pl.when(r > 0)
        def _():
            ret_copy(j, r - 1).start()

        left, right = times_lower(ws, g, 0, rows)
        put(ds, (rows, T0), c2[rows, T0] - left)
        put(ds, (rows, T1), c2[rows, T1] - right)
        left, right = times_lower(ds, fs2, 0, rows)
        put(zs2, (rows, T0), left)
        put(zs2, (rows, T1), right)
        low = times_lower(zs1, vs1, B, rows)
        upp = times_upper(zs2, vs2, rows)
        for i in range(2):
            cols = slice(256 * i, 256 * (i + 1))
            out[pl.ds(256 * i, 256), pl.ds(NC * j, NC)] = (xt[rows, cols] - low[i] - upp[i]).T

    for j in range(PARTS):
        rows = slice(NC * j, NC * (j + 1))

        @pl.when(r < last)
        def _():
            ret_copy(j, r).wait_recv()

        for k in range(STRIPES):
            stripe = slice(LC * k, LC * (k + 1))
            v = xt[rows, slice(B + LC * k, B + LC * (k + 1))] - do_buf[j, k] - ret_buf[j, :, stripe]
            out[pl.ds(B + LC * k, LC), pl.ds(NC * j, NC)] = v.T

    for done in sent:
        done()

    @pl.when(giver)
    def _():
        for k in range(2):
            for t in range(2):
                given(t, k).wait_send()

    @pl.when(r < last)
    def _():
        pltpu.make_async_remote_copy(
            src_ref=x_buf.at[pl.ds(B, B), :], dst_ref=xp_buf, send_sem=xc_s.at[0], recv_sem=xc_r.at[0],
            device_id=(c, r + 1), device_id_type=MESH,
        ).wait_send()
        for j in range(PARTS):
            for i in range(STRIPES):
                d_copy(j, i, r + 1).wait_send()

    @pl.when(r > 0)
    def _():
        for j in range(PARTS):
            ret_copy(j, r - 1).wait_send()


def body(vectors, reflectors, factors):
    vmem = pltpu.VMEM
    dma = pltpu.SemaphoreType.DMA
    pair = (2, N, B)
    square = (2, B, B)
    scratch = [
        vmem((2, NZ, NX, NH, 8, BAND), F32), vmem((2, NZ, NX, NH, 8, B), F32),
        vmem((2 * B, N), F32), vmem((B, N), F32),
        vmem((PARTS, STRIPES, NC, LC), F32), vmem((PARTS, STRIPES, NC, LC), F32),
        vmem((PARTS, NC, B), F32), vmem((PARTS, NC, B), F32),
        vmem((2, N, 3 * B), BF16),
        vmem((2, B, 2 * B), BF16), vmem((2, B, 2 * B), BF16),
        vmem(square, BF16), vmem(square, BF16),
        vmem(square, BF16), vmem(square, BF16), vmem(square, BF16), vmem(square, BF16), vmem(square, BF16),
        vmem(pair, BF16), vmem(pair, BF16), vmem(pair, BF16), vmem(pair, BF16),
        vmem((N, B), F32), vmem((N, B), F32), vmem((N, B), F32), vmem((N, 2 * B), F32),
        vmem((2, 2, 8, BAND), F32), vmem((2, 2, 8, B), F32), dma((2, 2, 2)),
        dma((5,)), dma((2, 2)), dma((2,)), dma((2, 4)), dma((2, 4)), dma((2, 2, NZ)), dma((2, 2, NZ)),
        dma((2, 2)), dma((2, 2)), dma((2, 2, 4)), dma((2, 2, 4)),
        dma((2, 2, NZ)), dma((2, 2, NZ)), dma((2, 4)), dma((2, 4)),
        dma((1,)), dma((1,)), dma((PARTS, STRIPES)), dma((PARTS, STRIPES)), dma((PARTS,)), dma((PARTS,)),
    ]
    return pl.pallas_call(
        kernel,
        out_shape=jax.ShapeDtypeStruct((2 * B, N), F32),
        in_specs=[pl.BlockSpec(memory_space=pl.ANY)] * 3,
        out_specs=pl.BlockSpec(memory_space=pltpu.VMEM),
        scratch_shapes=scratch,
        compiler_params=pltpu.CompilerParams(
            collective_id=0, has_side_effects=True, vmem_limit_bytes=56 << 20
        ),
    )(vectors, jnp.transpose(reflectors, (0, 2, 1)), jnp.transpose(factors, (0, 2, 1)))


def solution(mesh):
    placed = (P("rows", "cols"), P(None, None, "cols"), P(None, None, "cols"))
    return jax.shard_map(
        body, mesh=mesh, in_specs=placed, out_specs=P("rows", "cols"), check_vma=False
    )
```

```python
import jax
import jax.numpy as jnp
from jax import lax
from jax.experimental import pallas as pl
from jax.experimental.pallas import tpu as pltpu
from jax.sharding import PartitionSpec as P

MESH = pl.DeviceIdType.MESH
F32, BF16 = jnp.float32, jnp.bfloat16
NZ, NX, NH = 8, 4, 2
B, HALF, N = 512, 256, 256
BAND = 640
LC = 128
STRIPES = B // LC
PARTS = 2
NC = N // PARTS
NN = (((1,), (0,)), ((), ()))
NT = (((1,), (1,)), ((), ()))
TN = (((0,), (0,)), ((), ()))


def split(v):
    hi = v.astype(BF16)
    return hi, (v - hi.astype(F32)).astype(BF16)


def dot3(a, b, dims=NN):
    def one(u, v):
        return lax.dot_general(u, v, dims, preferred_element_type=F32)

    return one(a[0], b[0]) + one(a[0], b[1]) + one(a[1], b[0])


def put(ref, at, v):
    hi, lo = split(v)
    ref[(0, *at)] = hi
    ref[(1, *at)] = lo


def get(ref, rows, cols):
    return ref[0, rows, cols], ref[1, rows, cols]


ALL, T0, T1 = slice(0, 512), slice(0, 256), slice(256, 512)


def times_lower(a, m, off=0, rows=slice(None)):
    lo, hi = slice(off, off + 256), slice(off + 256, off + 512)
    left = dot3(get(a, rows, ALL), get(m, ALL, lo))
    right = dot3(get(a, rows, T1), get(m, T1, hi))
    return left, right


def times_upper(a, m, rows):
    left = dot3(get(a, rows, T0), get(m, T0, T0))
    right = dot3(get(a, rows, ALL), get(m, ALL, T1))
    return left, right


def lower_lower(out, a, m, off=0):
    lo, hi = slice(off, off + 256), slice(off + 256, off + 512)
    put(out, (T0, T0), dot3(get(a, T0, T0), get(m, T0, lo)))
    put(out, (T1, T0), dot3(get(a, T1, ALL), get(m, ALL, lo)))
    put(out, (T1, T1), dot3(get(a, T1, T1), get(m, T1, hi)))


def kernel(
    vec, rft, fat, out,
    vt_buf, ft_buf, x_buf, xp_buf, d_buf, do_buf, ret_buf, ro_buf,
    xs, vs1, vs2, fs1, fs2, h1, h2, g, m, at, ds, ws, zs1, zs2,
    c1, c2, e, xt,
    gv_buf, gf_buf, gsem, lsem, p_s, p_r, vz_s, vz_r, vx_s, vx_r, wx_s, wx_r, wz_s, wz_r, fx_s, fx_r, fz_s, fz_r,
    xc_s, xc_r, d_s, d_r, ret_s, ret_r,
):
    c = lax.axis_index("cols")
    r = lax.axis_index("rows")
    z, x, h = c // (NX * NH), (c // NH) % NX, c % NH
    q = z // 2
    last = lax.axis_size("rows") - 1

    def at_c(zz, xx, hh):
        return (zz * NX + xx) * NH + hh

    zp, zm = at_c((z + 1) % NZ, x, h), at_c((z + NZ - 1) % NZ, x, h)
    xp, xm = at_c(z, (x + 1) % NX, h), at_c(z, (x + NX - 1) % NX, h)
    twin = at_c(z, x, 1 - h)
    b_first, b_own = jnp.maximum(2 * r - 1, 0), 2 * r
    zdir, xdir = (zp, zm), (xp, xm)

    lanes = pl.ds(pl.multiple_of(128 * q, 128), BAND)
    local = []
    for i, b in enumerate((b_first, b_own)):
        local.append(pltpu.make_async_copy(rft.at[b, :, lanes], vt_buf.at[i, z, x, h], lsem.at[2 * i]))
        local.append(pltpu.make_async_copy(fat.at[b], ft_buf.at[i, z, x, h], lsem.at[2 * i + 1]))
    xload = pltpu.make_async_copy(vec, x_buf, lsem.at[4])
    for cp in local:
        cp.start()
    xload.start()

    y, core = r // 2, r % 2
    near = 2 * jnp.where(y < 2, 3, 0) + core
    giver = (y == 0) | (y == 3)
    takers = [2 * (jnp.where(y == 3, 0, 2) + t) + core for t in range(2)]

    def gift(t, i):
        b = 2 * takers[t] if i else jnp.maximum(2 * takers[t] - 1, 0)
        return (
            pltpu.make_async_copy(rft.at[b, :, lanes], gv_buf.at[t, i], gsem.at[t, i, 0]),
            pltpu.make_async_copy(fat.at[b], gf_buf.at[t, i], gsem.at[t, i, 1]),
        )

    def given(t, k):
        src, dst = (gv_buf, vt_buf) if k == 0 else (gf_buf, ft_buf)
        return pltpu.make_async_remote_copy(
            src_ref=src.at[t], dst_ref=dst.at[:, z, x, h], send_sem=p_s.at[t, k], recv_sem=p_r.at[k],
            device_id=(twin, takers[t]), device_id_type=MESH,
        )

    @pl.when(giver)
    def _():
        for t in range(2):
            for i in range(2):
                for cp in gift(t, i):
                    cp.start()

    barrier = pltpu.get_barrier_semaphore()
    for cc in (zp, zm, xp, xm):
        pl.semaphore_signal(barrier, inc=1, device_id=(cc, r), device_id_type=MESH)

    pl.semaphore_signal(barrier, inc=1, device_id=(twin, near), device_id_type=MESH)

    @pl.when(giver)
    def _():
        for t in range(2):
            pl.semaphore_signal(barrier, inc=1, device_id=(twin, takers[t]), device_id_type=MESH)

    @pl.when(r > 0)
    def _():
        pl.semaphore_signal(barrier, inc=1, device_id=(c, r - 1), device_id_type=MESH)

    @pl.when(r < last)
    def _():
        pl.semaphore_signal(barrier, inc=1, device_id=(c, r + 1), device_id_type=MESH)

    @pl.when(r == 0)
    def _():
        xp_buf[...] = jnp.zeros_like(xp_buf)
        d_buf[...] = jnp.zeros_like(d_buf)

    @pl.when(r == last)
    def _():
        ret_buf[...] = jnp.zeros_like(ret_buf)

    for i in range(2):
        vs = (vs1, vs2)[i]
        for qq in range(4):
            gap = (640, 0, 896, 256)[qq]
            for k in range(2):
                vs[k, pl.ds(128 * qq, 128), pl.ds(gap, 128)] = jnp.zeros((128, 128), BF16)
    for ref in (fs1, fs2):
        for k in range(2):
            ref[k, pl.ds(0, 128), pl.ds(128, 128)] = jnp.zeros((128, 128), BF16)
            ref[k, pl.ds(256, 128), pl.ds(384, 128)] = jnp.zeros((128, 128), BF16)
    for cp in local:
        cp.wait()
    xload.wait()
    for i in range(4):
        rows = pl.ds(256 * i, 256)
        v = x_buf[rows, :].T
        xt[:, rows] = v
        put(xs, (slice(None), pl.ds(B + 256 * i, 256)), v)

    @pl.when(giver)
    def _():
        for t in range(2):
            for i in range(2):
                for cp in gift(t, i):
                    cp.wait()

    peers = 5 + jnp.minimum(r, 1) + jnp.minimum(last - r, 1) + jnp.where(giver, 2, 0)
    pl.semaphore_wait(barrier, peers)

    @pl.when(giver)
    def _():
        for k in range(2):
            for t in range(2):
                given(t, k).start()

    sent = []

    def remote(ref, ssem, rsem, cc):
        return pltpu.make_async_remote_copy(
            src_ref=ref, dst_ref=ref, send_sem=ssem, recv_sem=rsem,
            device_id=(cc, r), device_id_type=MESH,
        )

    def send(ref, ssem, rsem, cc):
        cp = remote(ref, ssem, rsem, cc)
        cp.start()
        sent.append(cp.wait_send)

    def arrived(ref, ssem, rsem, cc):
        remote(ref, ssem, rsem, cc).wait_recv()

    def by_width(zz, do):
        for w in range(4):
            @pl.when(zz // 2 == w)
            def _(w=w):
                do(128 * (w + 1))

    def slab(dz):
        return (z + dz + NZ) % NZ

    both = slice(None)
    xnear = ((x + NX - 1) % NX, (x + 1) % NX)
    xfar = (x + 2) % NX

    def part(d):
        return pl.ds(d, 1)

    def vz_args(n, d, dz):
        half = both if n < 4 else part(d)
        return vt_buf.at[0, slab(dz), x, half], vz_s.at[d, n - 1], vz_r.at[d, n - 1], zdir[d]

    def vz_send(n):
        for d in range(2):
            send(*vz_args(n, d, (1 - n) if d == 0 else (n - 1)))

    def vz_step(n):
        for d in range(2):
            arrived(*vz_args(n, d, -n if d == 0 else n))
            if n < 4:
                send(*vz_args(n + 1, d, -n if d == 0 else n))

    def vx_args(dz, n, d, xx):
        half = both if n == 0 else part(d)
        k = dz % NZ
        return vt_buf.at[0, slab(dz), xx, half], vx_s.at[d, n, k], vx_r.at[d, n, k], xdir[d]

    def wx_args(n, d, xx):
        half = both if n == 0 else part(d)
        return vt_buf.at[1, z, xx, half], wx_s.at[d, n], wx_r.at[d, n], xdir[d]

    def wz_args(n, d, p, dz):
        return vt_buf.at[1, slab(dz), pl.ds(2 * p, 2)], wz_s.at[d, p, n - 1], wz_r.at[d, p, n - 1], zdir[d]

    def wz_step(n):
        for p in range(2):
            for d in range(2):
                if n == 4 and p != d:
                    continue
                dz = -n if d == 0 else n
                if n > 0:
                    arrived(*wz_args(n, d, p, dz))
                if n < 3 or (n == 3 and p == d):
                    send(*wz_args(n + 1, d, p, dz))

    def fz_args(n, d, dz):
        blk = both if n < 4 else part(d)
        return ft_buf.at[blk, slab(dz), x], fz_s.at[d, n - 1], fz_r.at[d, n - 1], zdir[d]

    def fz_send(n):
        for d in range(2):
            send(*fz_args(n, d, (1 - n) if d == 0 else (n - 1)))

    def fz_step(n):
        for d in range(2):
            arrived(*fz_args(n, d, -n if d == 0 else n))
            if n < 4:
                send(*fz_args(n + 1, d, -n if d == 0 else n))

    def fx(dz, n, d, xx, do):
        blk, k = both if n == 0 else part(d), dz % NZ

        def at_width(width):
            do(remote(
                ft_buf.at[blk, slab(dz), xx, :, :, pl.ds(0, width)],
                fx_s.at[d, n, k], fx_r.at[d, n, k], xdir[d],
            ))

        by_width(slab(dz), at_width)

    def fx_go(dz, n, d, xx):
        fx(dz, n, d, xx, lambda cp: cp.start())
        sent.append(lambda: fx(dz, n, d, xx, lambda cp: cp.wait_send()))

    def x_send1(*dzs):
        for dz in dzs:
            for d in range(2):
                send(*vx_args(dz, 0, d, x))

    def fx_send1(*dzs):
        for dz in dzs:
            for d in range(2):
                fx_go(dz, 0, d, x)

    def x_send2(*dzs):
        for dz in dzs:
            for d in range(2):
                arrived(*vx_args(dz, 0, d, xnear[d]))
                send(*vx_args(dz, 1, d, xnear[d]))

    def fx_send2(*dzs):
        for dz in dzs:
            for d in range(2):
                fx(dz, 0, d, xnear[d], lambda cp: cp.wait_recv())
                fx_go(dz, 1, d, xnear[d])

    def x_last(*dzs):
        for dz in dzs:
            for d in range(2):
                arrived(*vx_args(dz, 1, d, xfar))

    def fx_last(*dzs):
        for dz in dzs:
            for d in range(2):
                fx(dz, 1, d, xfar, lambda cp: cp.wait_recv())

    arrived(vt_buf.at[:, z, x, 1 - h], p_s.at[0, 0], p_r.at[0], twin)
    for d in range(2):
        send(*wx_args(0, d, x))
    vz_send(1)
    arrived(ft_buf.at[:, z, x, 1 - h], p_s.at[0, 1], p_r.at[1], twin)
    fz_send(1)
    x_send1(0)
    fx_send1(0)

    @pl.when(r < last)
    def _():
        pltpu.make_async_remote_copy(
            src_ref=x_buf.at[pl.ds(B, B), :], dst_ref=xp_buf, send_sem=xc_s.at[0], recv_sem=xc_r.at[0],
            device_id=(c, r + 1), device_id_type=MESH,
        ).start()

    for d in range(2):
        arrived(*wx_args(0, d, xnear[d]))
        send(*wx_args(1, d, xnear[d]))
    vz_step(1)
    fz_step(1)
    x_send1(-1, 1)
    fx_send1(-1, 1)
    for d in range(2):
        arrived(*wx_args(1, d, xfar))
    wz_step(0)
    vz_step(2)
    fz_step(2)
    x_send1(-2, 2)
    fx_send1(-2, 2)
    x_send2(0)
    fx_send2(0)
    wz_step(1)
    vz_step(3)
    fz_step(3)
    x_send1(-3, 3)
    fx_send1(-3, 3)
    x_send2(-1, 1)
    fx_send2(-1, 1)
    vz_step(4)
    fz_step(4)
    x_send1(4)
    fx_send1(4)
    wz_step(2)
    x_send2(-2, 2)
    fx_send2(-2, 2)
    wz_step(3)
    x_send2(-3, 3, 4)
    fx_send2(-3, 3, 4)

    @pl.when(r > 0)
    def _():
        pltpu.make_async_remote_copy(
            src_ref=x_buf.at[pl.ds(B, B), :], dst_ref=xp_buf, send_sem=xc_s.at[0], recv_sem=xc_r.at[0],
            device_id=(c, r), device_id_type=MESH,
        ).wait_recv()

    for i in range(2):
        put(xs, (slice(None), pl.ds(256 * i, 256)), xp_buf[pl.ds(256 * i, 256), :].T)
    has_upper = r > 0

    def unpack(i):
        vs = (vs1, vs2)[i]
        for qq in range(4):
            v = vt_buf[i, pl.ds(2 * qq, 2)].reshape(128, BAND)
            if i == 0:
                v = jnp.where(has_upper, v, jnp.zeros_like(v))
            put(vs, (pl.ds(128 * qq, 128), pl.ds(128 * qq, BAND)), v)

    def own_weights(i):
        cref, vs, off = ((c1, vs1, 0), (c2, vs2, B))[i]
        for a in range(2):
            w = pl.ds(256 * a, 768)
            cref[:, pl.ds(256 * a, 256)] = dot3(
                get(xs, slice(None), pl.ds(off + 256 * a, 768)), get(vs, pl.ds(256 * a, 256), w), NT
            )

    wz_step(4)
    unpack(1)
    own_weights(1)
    x_last(0, -1, 1, -2, 2, -3, 3, 4)
    unpack(0)
    own_weights(0)
    put(ws, (slice(None), slice(None)), c1[...])

    fx_last(0, -1, 1, -2, 2, -3, 3, 4)
    for fs, i in ((fs1, 0), (fs2, 1)):
        for qq in range(4):
            w = pl.ds(0, 128 * (qq + 1))
            v = ft_buf[i, pl.ds(2 * qq, 2), :, :, :, w].reshape(128, 128 * (qq + 1))
            put(fs, (pl.ds(128 * qq, 128), w), v)

    lower_lower(h1, fs1, vs1, B)
    lower_lower(h2, fs2, vs2, B)
    put(g, (T0, T0), dot3(get(h1, T0, T0), get(vs2, T0, T0), NT))
    put(g, (T1, T0), dot3(get(h1, T1, ALL), get(vs2, T0, ALL), NT))
    put(g, (T1, T1), dot3(get(h1, T1, T1), get(vs2, T1, T1), NT))
    lower_lower(m, g, h2)
    put(at, (T0, T0), dot3(get(vs1, T0, T0), get(m, T0, T0), TN))
    put(at, (T1, T0), dot3(get(vs1, ALL, T1), get(m, ALL, T0), TN))
    put(at, (T1, T1), dot3(get(vs1, T1, T1), get(m, T1, T1), TN))
    for k in range(2):
        at[k, T0, T1] = jnp.zeros((256, 256), BF16)
    left, right = times_lower(ws, g)
    put(ds, (slice(None), T0), c2[:, T0] - left)
    put(ds, (slice(None), T1), c2[:, T1] - right)
    left, right = times_lower(ds, h2)
    e[:, T0] = left
    e[:, T1] = right

    def d_copy(j, i, rr):
        return pltpu.make_async_remote_copy(
            src_ref=do_buf.at[j, i], dst_ref=d_buf.at[j, i], send_sem=d_s.at[j, i], recv_sem=d_r.at[j, i],
            device_id=(c, rr), device_id_type=MESH,
        )

    def ret_copy(j, rr):
        return pltpu.make_async_remote_copy(
            src_ref=ro_buf.at[j], dst_ref=ret_buf.at[j], send_sem=ret_s.at[j], recv_sem=ret_r.at[j],
            device_id=(c, rr), device_id_type=MESH,
        )

    for j in range(PARTS):
        rows = slice(NC * j, NC * (j + 1))
        acc = e[rows, slice(B - LC, B)]
        for i in reversed(range(STRIPES)):
            @pl.when(r > 0)
            def _(i=i):
                d_copy(j, i, r).wait_recv()

            stripe, rest = slice(LC * i, LC * (i + 1)), slice(LC * i, B)
            put(ds, (rows, stripe), d_buf[j, i])
            do_buf[j, i] = acc + dot3(get(ds, rows, stripe), get(at, stripe, stripe))

            @pl.when(r < last)
            def _(i=i):
                d_copy(j, i, r + 1).start()

            if i > 0:
                after = slice(LC * (i - 1), LC * i)
                acc = e[rows, after] + dot3(get(ds, rows, rest), get(at, rest, after))

        put(ws, (rows, T1), c1[rows, T1] - dot3(get(ds, rows, T1), get(vs1, T1, T1), NT))
        put(ws, (rows, T0), c1[rows, T0] - dot3(get(ds, rows, ALL), get(vs1, T0, ALL), NT))
        left, right = times_lower(ws, fs1, 0, rows)
        put(zs1, (rows, T0), left)
        put(zs1, (rows, T1), right)
        left, right = times_upper(zs1, vs1, rows)
        ro_buf[j, :, T0] = left
        ro_buf[j, :, T1] = right

        @pl.when(r > 0)
        def _():
            ret_copy(j, r - 1).start()

    for j in range(PARTS):
        rows = slice(NC * j, NC * (j + 1))
        left, right = times_lower(ws, g, 0, rows)
        put(ds, (rows, T0), c2[rows, T0] - left)
        put(ds, (rows, T1), c2[rows, T1] - right)
        left, right = times_lower(ds, fs2, 0, rows)
        put(zs2, (rows, T0), left)
        put(zs2, (rows, T1), right)
        low = times_lower(zs1, vs1, B, rows)
        upp = times_upper(zs2, vs2, rows)
        for i in range(2):
            cols = slice(256 * i, 256 * (i + 1))
            out[pl.ds(256 * i, 256), pl.ds(NC * j, NC)] = (xt[rows, cols] - low[i] - upp[i]).T

    for j in range(PARTS):
        rows = slice(NC * j, NC * (j + 1))

        @pl.when(r < last)
        def _():
            ret_copy(j, r).wait_recv()

        for k in range(STRIPES):
            stripe = slice(LC * k, LC * (k + 1))
            v = xt[rows, slice(B + LC * k, B + LC * (k + 1))] - do_buf[j, k] - ret_buf[j, :, stripe]
            out[pl.ds(B + LC * k, LC), pl.ds(NC * j, NC)] = v.T

    for done in sent:
        done()

    @pl.when(giver)
    def _():
        for k in range(2):
            for t in range(2):
                given(t, k).wait_send()

    @pl.when(r < last)
    def _():
        pltpu.make_async_remote_copy(
            src_ref=x_buf.at[pl.ds(B, B), :], dst_ref=xp_buf, send_sem=xc_s.at[0], recv_sem=xc_r.at[0],
            device_id=(c, r + 1), device_id_type=MESH,
        ).wait_send()
        for j in range(PARTS):
            for i in range(STRIPES):
                d_copy(j, i, r + 1).wait_send()

    @pl.when(r > 0)
    def _():
        for j in range(PARTS):
            ret_copy(j, r - 1).wait_send()


def body(vectors, reflectors, factors):
    vmem = pltpu.VMEM
    dma = pltpu.SemaphoreType.DMA
    pair = (2, N, B)
    square = (2, B, B)
    scratch = [
        vmem((2, NZ, NX, NH, 8, BAND), F32), vmem((2, NZ, NX, NH, 8, B), F32),
        vmem((2 * B, N), F32), vmem((B, N), F32),
        vmem((PARTS, STRIPES, NC, LC), F32), vmem((PARTS, STRIPES, NC, LC), F32),
        vmem((PARTS, NC, B), F32), vmem((PARTS, NC, B), F32),
        vmem((2, N, 3 * B), BF16),
        vmem((2, B, 2 * B), BF16), vmem((2, B, 2 * B), BF16),
        vmem(square, BF16), vmem(square, BF16),
        vmem(square, BF16), vmem(square, BF16), vmem(square, BF16), vmem(square, BF16), vmem(square, BF16),
        vmem(pair, BF16), vmem(pair, BF16), vmem(pair, BF16), vmem(pair, BF16),
        vmem((N, B), F32), vmem((N, B), F32), vmem((N, B), F32), vmem((N, 2 * B), F32),
        vmem((2, 2, 8, BAND), F32), vmem((2, 2, 8, B), F32), dma((2, 2, 2)),
        dma((5,)), dma((2, 2)), dma((2,)), dma((2, 4)), dma((2, 4)), dma((2, 2, NZ)), dma((2, 2, NZ)),
        dma((2, 2)), dma((2, 2)), dma((2, 2, 4)), dma((2, 2, 4)),
        dma((2, 2, NZ)), dma((2, 2, NZ)), dma((2, 4)), dma((2, 4)),
        dma((1,)), dma((1,)), dma((PARTS, STRIPES)), dma((PARTS, STRIPES)), dma((PARTS,)), dma((PARTS,)),
    ]
    return pl.pallas_call(
        kernel,
        out_shape=jax.ShapeDtypeStruct((2 * B, N), F32),
        in_specs=[pl.BlockSpec(memory_space=pl.ANY)] * 3,
        out_specs=pl.BlockSpec(memory_space=pltpu.VMEM),
        scratch_shapes=scratch,
        compiler_params=pltpu.CompilerParams(
            collective_id=0, has_side_effects=True, vmem_limit_bytes=56 << 20
        ),
    )(vectors, jnp.transpose(reflectors, (0, 2, 1)), jnp.transpose(factors, (0, 2, 1)))


def solution(mesh):
    placed = (P("rows", "cols"), P(None, None, "cols"), P(None, None, "cols"))
    return jax.shard_map(
        body, mesh=mesh, in_specs=placed, out_specs=P("rows", "cols"), check_vma=False
    )
```

```python
import jax
import jax.numpy as jnp
from jax import lax
from jax.experimental import pallas as pl
from jax.experimental.pallas import tpu as pltpu
from jax.sharding import PartitionSpec as P

MESH = pl.DeviceIdType.MESH
F32, BF16 = jnp.float32, jnp.bfloat16
NZ, NX, NH = 8, 4, 2
B, HALF, N = 512, 256, 256
BAND = 640
LC = 128
STRIPES = B // LC
PARTS = 2
NC = N // PARTS
NN = (((1,), (0,)), ((), ()))
NT = (((1,), (1,)), ((), ()))
TN = (((0,), (0,)), ((), ()))


def split(v):
    hi = v.astype(BF16)
    return hi, (v - hi.astype(F32)).astype(BF16)


def dot3(a, b, dims=NN):
    def one(u, v):
        return lax.dot_general(u, v, dims, preferred_element_type=F32)

    return one(a[0], b[0]) + one(a[0], b[1]) + one(a[1], b[0])


def put(ref, at, v):
    hi, lo = split(v)
    ref[(0, *at)] = hi
    ref[(1, *at)] = lo


def get(ref, rows, cols):
    return ref[0, rows, cols], ref[1, rows, cols]


ALL, T0, T1 = slice(0, 512), slice(0, 256), slice(256, 512)


def times_lower(a, m, off=0, rows=slice(None)):
    lo, hi = slice(off, off + 256), slice(off + 256, off + 512)
    left = dot3(get(a, rows, ALL), get(m, ALL, lo))
    right = dot3(get(a, rows, T1), get(m, T1, hi))
    return left, right


def times_upper(a, m, rows):
    left = dot3(get(a, rows, T0), get(m, T0, T0))
    right = dot3(get(a, rows, ALL), get(m, ALL, T1))
    return left, right


def lower_lower(out, a, m, off=0):
    lo, hi = slice(off, off + 256), slice(off + 256, off + 512)
    put(out, (T0, T0), dot3(get(a, T0, T0), get(m, T0, lo)))
    put(out, (T1, T0), dot3(get(a, T1, ALL), get(m, ALL, lo)))
    put(out, (T1, T1), dot3(get(a, T1, T1), get(m, T1, hi)))


def kernel(
    vec, rft, fat, out,
    vt_buf, ft_buf, x_buf, xp_buf, d_buf, do_buf, ret_buf, ro_buf,
    xs, vs1, vs2, fs1, fs2, h1, h2, g, m, at, ds, ws, zs1, zs2,
    c1, c2, e, xt,
    gv_buf, gf_buf, gsem, lsem, p_s, p_r, vz_s, vz_r, vx_s, vx_r, wx_s, wx_r, wz_s, wz_r, fx_s, fx_r, fz_s, fz_r,
    xc_s, xc_r, d_s, d_r, ret_s, ret_r,
):
    c = lax.axis_index("cols")
    r = lax.axis_index("rows")
    z, x, h = c // (NX * NH), (c // NH) % NX, c % NH
    q = z // 2
    last = lax.axis_size("rows") - 1

    def at_c(zz, xx, hh):
        return (zz * NX + xx) * NH + hh

    zp, zm = at_c((z + 1) % NZ, x, h), at_c((z + NZ - 1) % NZ, x, h)
    xp, xm = at_c(z, (x + 1) % NX, h), at_c(z, (x + NX - 1) % NX, h)
    twin = at_c(z, x, 1 - h)
    b_first, b_own = jnp.maximum(2 * r - 1, 0), 2 * r
    zdir, xdir = (zp, zm), (xp, xm)

    lanes = pl.ds(pl.multiple_of(128 * q, 128), BAND)
    local = []
    for i, b in enumerate((b_first, b_own)):
        local.append(pltpu.make_async_copy(rft.at[b, :, lanes], vt_buf.at[i, z, x, h], lsem.at[2 * i]))
        local.append(pltpu.make_async_copy(fat.at[b], ft_buf.at[i, z, x, h], lsem.at[2 * i + 1]))
    xload = pltpu.make_async_copy(vec, x_buf, lsem.at[4])
    for cp in local:
        cp.start()
    xload.start()

    y, core = r // 2, r % 2
    near = 2 * jnp.where(y < 2, 3, 0) + core
    giver = (y == 0) | (y == 3)
    takers = [2 * (jnp.where(y == 3, 0, 2) + t) + core for t in range(2)]

    def gift(t, i):
        b = 2 * takers[t] if i else jnp.maximum(2 * takers[t] - 1, 0)
        return (
            pltpu.make_async_copy(rft.at[b, :, lanes], gv_buf.at[t, i], gsem.at[t, i, 0]),
            pltpu.make_async_copy(fat.at[b], gf_buf.at[t, i], gsem.at[t, i, 1]),
        )

    def given(t, k):
        src, dst = (gv_buf, vt_buf) if k == 0 else (gf_buf, ft_buf)
        return pltpu.make_async_remote_copy(
            src_ref=src.at[t], dst_ref=dst.at[:, z, x, h], send_sem=p_s.at[t, k], recv_sem=p_r.at[k],
            device_id=(twin, takers[t]), device_id_type=MESH,
        )

    @pl.when(giver)
    def _():
        for t in range(2):
            for i in range(2):
                for cp in gift(t, i):
                    cp.start()

    barrier = pltpu.get_barrier_semaphore()
    for cc in (zp, zm, xp, xm):
        pl.semaphore_signal(barrier, inc=1, device_id=(cc, r), device_id_type=MESH)

    pl.semaphore_signal(barrier, inc=1, device_id=(twin, near), device_id_type=MESH)

    @pl.when(giver)
    def _():
        for t in range(2):
            pl.semaphore_signal(barrier, inc=1, device_id=(twin, takers[t]), device_id_type=MESH)

    @pl.when(r > 0)
    def _():
        pl.semaphore_signal(barrier, inc=1, device_id=(c, r - 1), device_id_type=MESH)

    @pl.when(r < last)
    def _():
        pl.semaphore_signal(barrier, inc=1, device_id=(c, r + 1), device_id_type=MESH)

    @pl.when(r == 0)
    def _():
        xp_buf[...] = jnp.zeros_like(xp_buf)
        d_buf[...] = jnp.zeros_like(d_buf)

    @pl.when(r == last)
    def _():
        ret_buf[...] = jnp.zeros_like(ret_buf)

    for i in range(2):
        vs = (vs1, vs2)[i]
        for qq in range(4):
            gap = (640, 0, 896, 256)[qq]
            for k in range(2):
                vs[k, pl.ds(128 * qq, 128), pl.ds(gap, 128)] = jnp.zeros((128, 128), BF16)
    for ref in (fs1, fs2):
        for k in range(2):
            ref[k, pl.ds(0, 128), pl.ds(128, 128)] = jnp.zeros((128, 128), BF16)
            ref[k, pl.ds(256, 128), pl.ds(384, 128)] = jnp.zeros((128, 128), BF16)
    for cp in local:
        cp.wait()
    xload.wait()
    for i in range(4):
        rows = pl.ds(256 * i, 256)
        v = x_buf[rows, :].T
        xt[:, rows] = v
        put(xs, (slice(None), pl.ds(B + 256 * i, 256)), v)

    @pl.when(giver)
    def _():
        for t in range(2):
            for i in range(2):
                for cp in gift(t, i):
                    cp.wait()

    peers = 5 + jnp.minimum(r, 1) + jnp.minimum(last - r, 1) + jnp.where(giver, 2, 0)
    pl.semaphore_wait(barrier, peers)

    @pl.when(giver)
    def _():
        for k in range(2):
            for t in range(2):
                given(t, k).start()

    sent = []

    def remote(ref, ssem, rsem, cc):
        return pltpu.make_async_remote_copy(
            src_ref=ref, dst_ref=ref, send_sem=ssem, recv_sem=rsem,
            device_id=(cc, r), device_id_type=MESH,
        )

    def send(ref, ssem, rsem, cc):
        cp = remote(ref, ssem, rsem, cc)
        cp.start()
        sent.append(cp.wait_send)

    def arrived(ref, ssem, rsem, cc):
        remote(ref, ssem, rsem, cc).wait_recv()

    def by_width(zz, do):
        for w in range(4):
            @pl.when(zz // 2 == w)
            def _(w=w):
                do(128 * (w + 1))

    def slab(dz):
        return (z + dz + NZ) % NZ

    both = slice(None)
    xnear = ((x + NX - 1) % NX, (x + 1) % NX)
    xfar = (x + 2) % NX

    def part(d):
        return pl.ds(d, 1)

    def vz_args(n, d, dz):
        half = both if n < 4 else part(d)
        return vt_buf.at[0, slab(dz), x, half], vz_s.at[d, n - 1], vz_r.at[d, n - 1], zdir[d]

    def vz_send(n):
        for d in range(2):
            send(*vz_args(n, d, (1 - n) if d == 0 else (n - 1)))

    def vz_step(n):
        for d in range(2):
            arrived(*vz_args(n, d, -n if d == 0 else n))
            if n < 4:
                send(*vz_args(n + 1, d, -n if d == 0 else n))

    def vx_args(dz, n, d, xx):
        half = both if n == 0 else part(d)
        k = dz % NZ
        return vt_buf.at[0, slab(dz), xx, half], vx_s.at[d, n, k], vx_r.at[d, n, k], xdir[d]

    def wx_args(n, d, xx):
        half = both if n == 0 else part(d)
        return vt_buf.at[1, z, xx, half], wx_s.at[d, n], wx_r.at[d, n], xdir[d]

    def wz_args(n, d, p, dz):
        return vt_buf.at[1, slab(dz), pl.ds(2 * p, 2)], wz_s.at[d, p, n - 1], wz_r.at[d, p, n - 1], zdir[d]

    def wz_step(n):
        for p in range(2):
            for d in range(2):
                if n == 4 and p != d:
                    continue
                dz = -n if d == 0 else n
                if n > 0:
                    arrived(*wz_args(n, d, p, dz))
                if n < 3 or (n == 3 and p == d):
                    send(*wz_args(n + 1, d, p, dz))

    def fz_args(n, d, dz):
        blk = both if n < 4 else part(d)
        return ft_buf.at[blk, slab(dz), x], fz_s.at[d, n - 1], fz_r.at[d, n - 1], zdir[d]

    def fz_send(n):
        for d in range(2):
            send(*fz_args(n, d, (1 - n) if d == 0 else (n - 1)))

    def fz_step(n):
        for d in range(2):
            arrived(*fz_args(n, d, -n if d == 0 else n))
            if n < 4:
                send(*fz_args(n + 1, d, -n if d == 0 else n))

    def fx(dz, n, d, xx, do):
        blk, k = both if n == 0 else part(d), dz % NZ

        def at_width(width):
            do(remote(
                ft_buf.at[blk, slab(dz), xx, :, :, pl.ds(0, width)],
                fx_s.at[d, n, k], fx_r.at[d, n, k], xdir[d],
            ))

        by_width(slab(dz), at_width)

    def fx_go(dz, n, d, xx):
        fx(dz, n, d, xx, lambda cp: cp.start())
        sent.append(lambda: fx(dz, n, d, xx, lambda cp: cp.wait_send()))

    def x_send1(*dzs):
        for dz in dzs:
            for d in range(2):
                send(*vx_args(dz, 0, d, x))

    def fx_send1(*dzs):
        for dz in dzs:
            for d in range(2):
                fx_go(dz, 0, d, x)

    def x_send2(*dzs):
        for dz in dzs:
            for d in range(2):
                arrived(*vx_args(dz, 0, d, xnear[d]))
                send(*vx_args(dz, 1, d, xnear[d]))

    def fx_send2(*dzs):
        for dz in dzs:
            for d in range(2):
                fx(dz, 0, d, xnear[d], lambda cp: cp.wait_recv())
                fx_go(dz, 1, d, xnear[d])

    def x_last(*dzs):
        for dz in dzs:
            for d in range(2):
                arrived(*vx_args(dz, 1, d, xfar))

    def fx_last(*dzs):
        for dz in dzs:
            for d in range(2):
                fx(dz, 1, d, xfar, lambda cp: cp.wait_recv())

    arrived(vt_buf.at[:, z, x, 1 - h], p_s.at[0, 0], p_r.at[0], twin)
    for d in range(2):
        send(*wx_args(0, d, x))
    vz_send(1)
    arrived(ft_buf.at[:, z, x, 1 - h], p_s.at[0, 1], p_r.at[1], twin)
    fz_send(1)
    x_send1(0)
    fx_send1(0)

    @pl.when(r < last)
    def _():
        pltpu.make_async_remote_copy(
            src_ref=x_buf.at[pl.ds(B, B), :], dst_ref=xp_buf, send_sem=xc_s.at[0], recv_sem=xc_r.at[0],
            device_id=(c, r + 1), device_id_type=MESH,
        ).start()

    for d in range(2):
        arrived(*wx_args(0, d, xnear[d]))
        send(*wx_args(1, d, xnear[d]))
    vz_step(1)
    fz_step(1)
    x_send1(-1, 1)
    fx_send1(-1, 1)
    for d in range(2):
        arrived(*wx_args(1, d, xfar))
    wz_step(0)
    vz_step(2)
    fz_step(2)
    x_send1(-2, 2)
    fx_send1(-2, 2)
    x_send2(0)
    fx_send2(0)
    wz_step(1)
    vz_step(3)
    fz_step(3)
    x_send1(-3, 3)
    fx_send1(-3, 3)
    x_send2(-1, 1)
    fx_send2(-1, 1)
    vz_step(4)
    fz_step(4)
    x_send1(4)
    fx_send1(4)
    wz_step(2)
    x_send2(-2, 2)
    fx_send2(-2, 2)
    wz_step(3)
    x_send2(-3, 3, 4)
    fx_send2(-3, 3, 4)

    @pl.when(r > 0)
    def _():
        pltpu.make_async_remote_copy(
            src_ref=x_buf.at[pl.ds(B, B), :], dst_ref=xp_buf, send_sem=xc_s.at[0], recv_sem=xc_r.at[0],
            device_id=(c, r), device_id_type=MESH,
        ).wait_recv()

    for i in range(2):
        put(xs, (slice(None), pl.ds(256 * i, 256)), xp_buf[pl.ds(256 * i, 256), :].T)
    has_upper = r > 0

    def unpack(i):
        vs = (vs1, vs2)[i]
        for qq in range(4):
            v = vt_buf[i, pl.ds(2 * qq, 2)].reshape(128, BAND)
            if i == 0:
                v = jnp.where(has_upper, v, jnp.zeros_like(v))
            put(vs, (pl.ds(128 * qq, 128), pl.ds(128 * qq, BAND)), v)

    def own_weights(i):
        cref, vs, off = ((c1, vs1, 0), (c2, vs2, B))[i]
        for a in range(2):
            w = pl.ds(256 * a, 768)
            cref[:, pl.ds(256 * a, 256)] = dot3(
                get(xs, slice(None), pl.ds(off + 256 * a, 768)), get(vs, pl.ds(256 * a, 256), w), NT
            )

    wz_step(4)
    unpack(1)
    own_weights(1)
    x_last(0, -1, 1, -2, 2, -3, 3, 4)
    unpack(0)
    own_weights(0)
    put(ws, (slice(None), slice(None)), c1[...])

    fx_last(0, -1, 1, -2, 2, -3, 3, 4)
    for fs, i in ((fs1, 0), (fs2, 1)):
        for qq in range(4):
            w = pl.ds(0, 128 * (qq + 1))
            v = ft_buf[i, pl.ds(2 * qq, 2), :, :, :, w].reshape(128, 128 * (qq + 1))
            put(fs, (pl.ds(128 * qq, 128), w), v)

    lower_lower(h1, fs1, vs1, B)
    lower_lower(h2, fs2, vs2, B)
    put(g, (T0, T0), dot3(get(h1, T0, T0), get(vs2, T0, T0), NT))
    put(g, (T1, T0), dot3(get(h1, T1, ALL), get(vs2, T0, ALL), NT))
    put(g, (T1, T1), dot3(get(h1, T1, T1), get(vs2, T1, T1), NT))
    left, right = times_lower(ws, g)
    put(ds, (slice(None), T0), c2[:, T0] - left)
    put(ds, (slice(None), T1), c2[:, T1] - right)
    left, right = times_lower(ds, h2)
    e[:, T0] = left
    e[:, T1] = right

    def d_copy(j, i, rr):
        return pltpu.make_async_remote_copy(
            src_ref=do_buf.at[j, i], dst_ref=d_buf.at[j, i], send_sem=d_s.at[j, i], recv_sem=d_r.at[j, i],
            device_id=(c, rr), device_id_type=MESH,
        )

    def ret_copy(j, rr):
        return pltpu.make_async_remote_copy(
            src_ref=ro_buf.at[j], dst_ref=ret_buf.at[j], send_sem=ret_s.at[j], recv_sem=ret_r.at[j],
            device_id=(c, rr), device_id_type=MESH,
        )

    @pl.when(r == 0)
    def _():
        for j in range(PARTS):
            for i in reversed(range(STRIPES)):
                do_buf[j, i] = e[slice(NC * j, NC * (j + 1)), slice(LC * i, LC * (i + 1))]
                d_copy(j, i, r + 1).start()

    lower_lower(m, g, h2)
    put(at, (T0, T0), dot3(get(vs1, T0, T0), get(m, T0, T0), TN))
    put(at, (T1, T0), dot3(get(vs1, ALL, T1), get(m, ALL, T0), TN))
    put(at, (T1, T1), dot3(get(vs1, T1, T1), get(m, T1, T1), TN))
    for k in range(2):
        at[k, T0, T1] = jnp.zeros((256, 256), BF16)

    for j in range(PARTS):
        rows = slice(NC * j, NC * (j + 1))
        acc = e[rows, slice(B - LC, B)]
        for i in reversed(range(STRIPES)):
            @pl.when(r > 0)
            def _(i=i):
                d_copy(j, i, r).wait_recv()

            stripe, rest = slice(LC * i, LC * (i + 1)), slice(LC * i, B)
            put(ds, (rows, stripe), d_buf[j, i])
            total = acc + dot3(get(ds, rows, stripe), get(at, stripe, stripe))

            @pl.when(r > 0)
            def _(i=i, total=total):
                do_buf[j, i] = total

            @pl.when((r > 0) & (r < last))
            def _(i=i):
                d_copy(j, i, r + 1).start()

            if i > 0:
                after = slice(LC * (i - 1), LC * i)
                acc = e[rows, after] + dot3(get(ds, rows, rest), get(at, rest, after))

        put(ws, (rows, T1), c1[rows, T1] - dot3(get(ds, rows, T1), get(vs1, T1, T1), NT))
        put(ws, (rows, T0), c1[rows, T0] - dot3(get(ds, rows, ALL), get(vs1, T0, ALL), NT))
        left, right = times_lower(ws, fs1, 0, rows)
        put(zs1, (rows, T0), left)
        put(zs1, (rows, T1), right)
        left, right = times_upper(zs1, vs1, rows)
        ro_buf[j, :, T0] = left
        ro_buf[j, :, T1] = right

        @pl.when(r > 0)
        def _():
            ret_copy(j, r - 1).start()

    for j in range(PARTS):
        rows = slice(NC * j, NC * (j + 1))
        left, right = times_lower(ws, g, 0, rows)
        put(ds, (rows, T0), c2[rows, T0] - left)
        put(ds, (rows, T1), c2[rows, T1] - right)
        left, right = times_lower(ds, fs2, 0, rows)
        put(zs2, (rows, T0), left)
        put(zs2, (rows, T1), right)
        low = times_lower(zs1, vs1, B, rows)
        upp = times_upper(zs2, vs2, rows)
        for i in range(2):
            cols = slice(256 * i, 256 * (i + 1))
            out[pl.ds(256 * i, 256), pl.ds(NC * j, NC)] = (xt[rows, cols] - low[i] - upp[i]).T

    for j in range(PARTS):
        rows = slice(NC * j, NC * (j + 1))

        @pl.when(r < last)
        def _():
            ret_copy(j, r).wait_recv()

        for k in range(STRIPES):
            stripe = slice(LC * k, LC * (k + 1))
            v = xt[rows, slice(B + LC * k, B + LC * (k + 1))] - do_buf[j, k] - ret_buf[j, :, stripe]
            out[pl.ds(B + LC * k, LC), pl.ds(NC * j, NC)] = v.T

    for done in sent:
        done()

    @pl.when(giver)
    def _():
        for k in range(2):
            for t in range(2):
                given(t, k).wait_send()

    @pl.when(r < last)
    def _():
        pltpu.make_async_remote_copy(
            src_ref=x_buf.at[pl.ds(B, B), :], dst_ref=xp_buf, send_sem=xc_s.at[0], recv_sem=xc_r.at[0],
            device_id=(c, r + 1), device_id_type=MESH,
        ).wait_send()
        for j in range(PARTS):
            for i in range(STRIPES):
                d_copy(j, i, r + 1).wait_send()

    @pl.when(r > 0)
    def _():
        for j in range(PARTS):
            ret_copy(j, r - 1).wait_send()


def body(vectors, reflectors, factors):
    vmem = pltpu.VMEM
    dma = pltpu.SemaphoreType.DMA
    pair = (2, N, B)
    square = (2, B, B)
    scratch = [
        vmem((2, NZ, NX, NH, 8, BAND), F32), vmem((2, NZ, NX, NH, 8, B), F32),
        vmem((2 * B, N), F32), vmem((B, N), F32),
        vmem((PARTS, STRIPES, NC, LC), F32), vmem((PARTS, STRIPES, NC, LC), F32),
        vmem((PARTS, NC, B), F32), vmem((PARTS, NC, B), F32),
        vmem((2, N, 3 * B), BF16),
        vmem((2, B, 2 * B), BF16), vmem((2, B, 2 * B), BF16),
        vmem(square, BF16), vmem(square, BF16),
        vmem(square, BF16), vmem(square, BF16), vmem(square, BF16), vmem(square, BF16), vmem(square, BF16),
        vmem(pair, BF16), vmem(pair, BF16), vmem(pair, BF16), vmem(pair, BF16),
        vmem((N, B), F32), vmem((N, B), F32), vmem((N, B), F32), vmem((N, 2 * B), F32),
        vmem((2, 2, 8, BAND), F32), vmem((2, 2, 8, B), F32), dma((2, 2, 2)),
        dma((5,)), dma((2, 2)), dma((2,)), dma((2, 4)), dma((2, 4)), dma((2, 2, NZ)), dma((2, 2, NZ)),
        dma((2, 2)), dma((2, 2)), dma((2, 2, 4)), dma((2, 2, 4)),
        dma((2, 2, NZ)), dma((2, 2, NZ)), dma((2, 4)), dma((2, 4)),
        dma((1,)), dma((1,)), dma((PARTS, STRIPES)), dma((PARTS, STRIPES)), dma((PARTS,)), dma((PARTS,)),
    ]
    return pl.pallas_call(
        kernel,
        out_shape=jax.ShapeDtypeStruct((2 * B, N), F32),
        in_specs=[pl.BlockSpec(memory_space=pl.ANY)] * 3,
        out_specs=pl.BlockSpec(memory_space=pltpu.VMEM),
        scratch_shapes=scratch,
        compiler_params=pltpu.CompilerParams(
            collective_id=0, has_side_effects=True, vmem_limit_bytes=56 << 20
        ),
    )(vectors, jnp.transpose(reflectors, (0, 2, 1)), jnp.transpose(factors, (0, 2, 1)))


def solution(mesh):
    placed = (P("rows", "cols"), P(None, None, "cols"), P(None, None, "cols"))
    return jax.shard_map(
        body, mesh=mesh, in_specs=placed, out_specs=P("rows", "cols"), check_vma=False
    )
```
